256 devices in a mesh: wall: 8 (over z), span: 32 (over x, y, core).
Axes of the slice: x: 4, y: 4, z: 8, core: 2. Of those that a mesh axis runs over, the one named last changes fastest.
Arguments:
- noise_bits: int32 [3, 32, 2048, 2048], P(None, None, 'span', 'wall'), may hold values from 0 to 1073741823
- filter_widths: int32 [2048], P('wall'), may hold values from 8 to 64, as said below
- target_mean_profile: float32 [3, 2048], P(None, 'wall'), may hold values from -4 to 4
- target_factor_diagonal: float32 [3, 2048], P(None, 'wall'), may hold values from 0.3 to 2
- target_factor_lower: float32 [3, 2048], P(None, 'wall'), may hold values from -0.8 to 0.8
Outputs:
- inflow_field: float32 [3, 32, 2048, 2048], P(None, None, 'span', 'wall')
The draws below stay inside these ranges and needn't reach their ends.
Inputs may be any that keep to these rules, and one draw needn't show every extreme that they name: `filter_widths`: every row's width lies between 8 and 64, and both ends occur in every draw.
All inputs are finite; a program needn't handle non-finite values.
Results may differ from the reference program's by a relative error of at most 0.0045.
Values may be sent and summed in bfloat16 or wider, within the bound.
A program may use at most 64 MiB of HBM per device.

```python
import math
import jax
import jax.numpy as jnp
from jax import lax

NC = 3
SAMPLES = 32
ROWS_PER_UNIT = 256
COLS_DEV = 64
WMAX = 64
SPANW = 32
TSCALE = 8
NY = 2048
NZ = 2048
N_WALL = 8


def draw_filter_widths(key, part):
    lowest = WMAX // 8
    sampled = jax.random.randint(key, (NY,), lowest, WMAX + 1)
    chosen = jax.random.randint(jax.random.fold_in(key, 7), (), 0, NY)
    sampled = sampled.at[chosen].set(WMAX)
    partner = (chosen + NY // 2) % NY
    return sampled.at[partner].set(lowest).astype(jnp.int32)


def place_ends(drawn, own_key, low, top_value):
    place = [jax.random.randint(jax.random.fold_in(own_key, axis), (), 0, length) for axis, length in enumerate(drawn.shape)]
    longest = drawn.shape.index(max(drawn.shape))
    beside = place[:longest] + [(place[longest] + 1) % drawn.shape[longest]] + place[longest + 1:]
    return drawn.at[tuple(place)].set(low).at[tuple(beside)].set(top_value)


def levels(own_key, shape, split, least, high):
    def one(position, blocks):
        steps = jax.random.uniform(jax.random.fold_in(jax.random.fold_in(own_key, 6), position), (blocks,), jnp.float32, least / len(split), high / len(split))
        return jnp.repeat(jnp.exp(steps), shape[position] // blocks).reshape((-1,) + (1,) * (len(shape) - position - 1))

    loudness = one(*split[0])
    for cut in split[1:]:
        loudness = loudness * one(*cut)
    return loudness


def gaussian(key, extent, scale, most, cuts=(), dtype=jnp.bfloat16):
    entries = scale * jax.random.normal(key, extent, jnp.float32)
    if cuts:
        entries = entries * levels(key, extent, cuts, -0.22, 0.18)
    return jnp.clip(entries, -most, most).astype(dtype)


def setup_inputs(seed: int = 0) -> dict:
    keys = jax.random.split(jax.random.key(seed), 6)
    return {
        "noise_bits": place_ends(jax.random.randint(keys[0], (NC, SAMPLES, NZ, NY), 0, 1073741824), jax.random.fold_in(keys[0], 1), 0, 1073741823).astype(jnp.int32),
        "filter_widths": draw_filter_widths(jax.random.fold_in(keys[5], 71), 0),
        "target_mean_profile": gaussian(keys[2], (NC, NY), 1.0, 4.0, ((1, 8),), jnp.float32),
        "target_factor_diagonal": jnp.clip(jnp.exp(math.log(2.0) - 1.89712 * jax.random.uniform(keys[3], (NC, NY), jnp.float32) ** levels(keys[3], (NC, NY), ((1, 8),), -0.2, 0.2)), 0.3, 2.0),
        "target_factor_lower": jnp.clip(jax.random.uniform(keys[4], (NC, NY), jnp.float32, -0.8, 0.8) * levels(keys[4], (NC, NY), ((1, 8),), -0.4, 0.0), -0.8, 0.8),
    }


PAIRS = ((0, 0), (1, 0), (1, 1), (2, 0), (2, 1), (2, 2))
SPREAD_FLOOR = 0.25
INV_RANGE = 1.0 / 1073741824.0

def to_field(noise_bits):
    scaled = (noise_bits.astype(jnp.float32) + 0.5) * INV_RANGE - 0.5
    return (math.sqrt(12.0) * scaled).astype(jnp.bfloat16)

def band_matrix(cell_widths, in_count, margin):
    out_count = cell_widths.shape[0]
    offsets = (lax.broadcasted_iota(jnp.int32, (out_count, in_count), 1) - margin - lax.broadcasted_iota(jnp.int32, (out_count, in_count), 0)).astype(jnp.float32)
    spread = cell_widths[:, None]
    inside = jnp.abs(offsets) <= 2.0 * spread
    safe_off = jnp.where(inside, offsets, 0.0)
    kernel = jnp.where(inside, jnp.exp(-math.pi * safe_off * safe_off / (8.0 * spread * spread)), 0.0)
    norm_total = jnp.sqrt(lax.optimization_barrier(jnp.sum(kernel * kernel, axis=1, keepdims=True)))
    return (kernel / norm_total).astype(jnp.bfloat16)

def time_matrix(sample_count):
    later_idx = lax.broadcasted_iota(jnp.int32, (sample_count, sample_count), 0)
    earlier = lax.broadcasted_iota(jnp.int32, (sample_count, sample_count), 1)
    causal = later_idx >= earlier
    lagged = jnp.where(causal, later_idx - earlier, 0).astype(jnp.float32)
    decay_rate = math.exp(-math.pi / (2.0 * TSCALE))
    fresh_gain = jnp.where(earlier == 0, 1.0, math.sqrt(1.0 - decay_rate * decay_rate))
    return jnp.where(causal, jnp.exp(-math.pi * lagged / (2.0 * TSCALE)) * fresh_gain, 0.0).astype(jnp.float32)

def lund_transform(sample_covariance, target_factor_diagonal, target_factor_lower):
    cov_00 = sample_covariance[0] + SPREAD_FLOOR
    cov_10 = sample_covariance[1]
    cov_11 = sample_covariance[2] + SPREAD_FLOOR
    cov_20 = sample_covariance[3]
    cov_21 = sample_covariance[4]
    cov_22 = sample_covariance[5] + SPREAD_FLOOR
    chol_00 = jnp.sqrt(cov_00)
    chol_10 = cov_10 / chol_00
    chol_20 = cov_20 / chol_00
    chol_11 = jnp.sqrt(cov_11 - chol_10 * chol_10)
    chol_21 = (cov_21 - chol_20 * chol_10) / chol_11
    chol_22 = jnp.sqrt(cov_22 - chol_20 * chol_20 - chol_21 * chol_21)
    inv_00 = 1.0 / chol_00
    inv_11 = 1.0 / chol_11
    inv_22 = 1.0 / chol_22
    inv_10 = -chol_10 * inv_00 * inv_11
    inv_21 = -chol_21 * inv_11 * inv_22
    inv_20 = -(chol_20 * inv_00 + chol_21 * inv_10) * inv_22
    gain_00 = target_factor_diagonal[0] * inv_00
    gain_10 = target_factor_lower[0] * inv_00 + target_factor_diagonal[1] * inv_10
    gain_11 = target_factor_diagonal[1] * inv_11
    gain_20 = target_factor_lower[1] * inv_00 + target_factor_lower[2] * inv_10 + target_factor_diagonal[2] * inv_20
    gain_21 = target_factor_lower[2] * inv_11 + target_factor_diagonal[2] * inv_21
    gain_22 = target_factor_diagonal[2] * inv_22
    return jnp.stack([gain_00, gain_10, gain_11, gain_20, gain_21, gain_22])

def rescaled_inflow(fluctuation, per_row_means, scaling_terms, velocity_profile):
    centred_samples = fluctuation - per_row_means[:, None, None, :]
    first_component = velocity_profile[0] + scaling_terms[0] * centred_samples[0]
    second_component = velocity_profile[1] + scaling_terms[1] * centred_samples[0] + scaling_terms[2] * centred_samples[1]
    third_component = velocity_profile[2] + scaling_terms[3] * centred_samples[0] + scaling_terms[4] * centred_samples[1] + scaling_terms[5] * centred_samples[2]
    return jnp.stack([first_component, second_component, third_component])

def reference(noise_bits, filter_widths, target_mean_profile, target_factor_diagonal, target_factor_lower):
    margin = 2 * WMAX
    span_margin = 2 * SPANW
    psi_field = to_field(noise_bits)
    padded = jnp.pad(psi_field, ((0, 0), (0, 0), (0, 0), (margin, margin)))
    span_band = band_matrix(jnp.full((COLS_DEV,), float(SPANW), jnp.float32), COLS_DEV + 2 * span_margin, span_margin).astype(jnp.float32)
    memory = time_matrix(SAMPLES)
    cell_count = float(SAMPLES * NZ)

    def one_block(block_idx, output):
        first_row_index = (block_idx * ROWS_PER_UNIT).astype(jnp.int32)
        window = lax.dynamic_slice_in_dim(padded, first_row_index, ROWS_PER_UNIT + 2 * margin, 3)
        row_widths = lax.dynamic_slice_in_dim(filter_widths, first_row_index, ROWS_PER_UNIT, 0)
        wall_band = band_matrix(row_widths.astype(jnp.float32), ROWS_PER_UNIT + 2 * margin, margin)
        smooth = jnp.einsum('csjm,ym->csjy', window.astype(jnp.float32), wall_band.astype(jnp.float32)).astype(jnp.bfloat16)
        blocks = smooth.reshape(NC, SAMPLES, NZ // COLS_DEV, COLS_DEV, ROWS_PER_UNIT)
        left_edge = jnp.roll(blocks, 1, axis=2)[:, :, :, COLS_DEV - span_margin:]
        right_edge = jnp.roll(blocks, -1, axis=2)[:, :, :, :span_margin]
        widened = jnp.concatenate([left_edge, blocks, right_edge], axis=3).astype(jnp.float32)
        spanned = jnp.einsum('kj,csbjy->csbky', span_band, widened).reshape(NC, SAMPLES, NZ, ROWS_PER_UNIT)
        fluctuation = jnp.einsum('ts,csky->ctky', memory, spanned, precision=lax.Precision.HIGHEST)
        per_row_means = lax.optimization_barrier(jnp.sum(fluctuation, axis=(1, 2))) / cell_count
        centred_samples = fluctuation - per_row_means[:, None, None, :]
        sample_covariance = jnp.stack([lax.optimization_barrier(jnp.sum(centred_samples[first_c] * centred_samples[second_c], axis=(0, 1))) for first_c, second_c in PAIRS]) / cell_count
        scaling_terms = lund_transform(sample_covariance, lax.dynamic_slice_in_dim(target_factor_diagonal, first_row_index, ROWS_PER_UNIT, 1), lax.dynamic_slice_in_dim(target_factor_lower, first_row_index, ROWS_PER_UNIT, 1))
        final_result = rescaled_inflow(fluctuation, per_row_means, scaling_terms, lax.dynamic_slice_in_dim(target_mean_profile, first_row_index, ROWS_PER_UNIT, 1))
        return lax.dynamic_update_slice_in_dim(output, final_result, first_row_index, 3)
    output = jnp.zeros((NC, SAMPLES, NZ, NY), jnp.float32)
    return lax.fori_loop(0, N_WALL, one_block, output)
```

```python
import functools
import math

import jax
import jax.numpy as jnp
from jax import lax
from jax.experimental import pallas as pl
from jax.experimental.pallas import tpu as pltpu
from jax.sharding import PartitionSpec as P

WMAX = 64
SPANW = 32
TSCALE = 8
STEP = 2
LAG = 3

PAIRS = ((0, 0), (1, 0), (1, 1), (2, 0), (2, 1), (2, 2))
SPREAD_FLOOR = 0.25
INV_RANGE = 1.0 / 1073741824.0
DECAY = math.exp(-math.pi / (2.0 * TSCALE))
FRESH = math.sqrt(1.0 - DECAY * DECAY)
MESH = pl.DeviceIdType.MESH


def raw_taps(offsets, spread):
    inside = jnp.abs(offsets) <= 2.0 * spread
    safe_off = jnp.where(inside, offsets, 0.0)
    return jnp.where(
        inside, jnp.exp(-math.pi * safe_off * safe_off / (8.0 * spread * spread)), 0.0
    )


def wall_bands(widths_ref, raw_ref, own_ref, edge_ref):
    n_rows = widths_ref.shape[1]
    margin = 2 * WMAX
    block = 64
    count = (n_rows + 2 * margin) // block
    spread = widths_ref[...].astype(jnp.float32)

    def fill(i, total):
        at = pl.multiple_of(i * block, block)
        row = lax.broadcasted_iota(jnp.int32, (block, n_rows), 0) + i * block
        col = lax.broadcasted_iota(jnp.int32, (block, n_rows), 1)
        taps = raw_taps((row - margin - col).astype(jnp.float32), spread)
        raw_ref[pl.ds(at, block), :] = taps
        return total + jnp.sum(taps * taps, axis=0, keepdims=True)

    total = lax.fori_loop(0, count, fill, jnp.zeros((1, n_rows), jnp.float32))
    norm = jnp.sqrt(total)
    edge_ref[:margin, :] = (raw_ref[:margin, :] / norm).astype(jnp.bfloat16)
    own_ref[...] = (raw_ref[margin : margin + n_rows, :] / norm).astype(jnp.bfloat16)
    edge_ref[margin:, :] = (raw_ref[margin + n_rows :, :] / norm).astype(jnp.bfloat16)


def span_band(band_ref):
    n_cols, in_count = band_ref.shape
    margin = 2 * SPANW
    row = lax.broadcasted_iota(jnp.int32, (n_cols, in_count), 0)
    col = lax.broadcasted_iota(jnp.int32, (n_cols, in_count), 1)
    taps = raw_taps((col - margin - row).astype(jnp.float32), float(SPANW))
    norm = jnp.sqrt(jnp.sum(taps * taps, axis=1, keepdims=True))
    band_ref[...] = (taps / norm).astype(jnp.bfloat16)


def filter_kernel(
    n_wall, n_span, noise, widths, fluct, totals,
    stage, psi, halo, smooth, from_left, from_right, raw, own_band, edge_band, z_band,
    carry, acc, sums,
    load_sem, wall_send, wall_recv, span_send, span_recv, sum_send, sum_recv,
):
    n_comp, _, n_cols, n_rows = noise.shape
    chunks = stage.shape[0]
    half = n_rows // 2
    rows = n_comp * STEP * n_cols
    w = lax.axis_index("wall")
    p = lax.axis_index("span")
    left, right = lax.rem(p + n_span - 1, n_span), lax.rem(p + 1, n_span)
    below, above = w > 0, w < n_wall - 1

    barrier = pltpu.get_barrier_semaphore()

    def greet(i, _):
        pl.semaphore_signal(
            barrier, inc=1, device_id={"span": lax.rem(p + i, n_span)}, device_id_type=MESH
        )
        return 0

    lax.fori_loop(1, n_span, greet, 0)

    @pl.when(below)
    def _():
        pl.semaphore_signal(barrier, inc=1, device_id={"wall": w - 1}, device_id_type=MESH)

    @pl.when(above)
    def _():
        pl.semaphore_signal(barrier, inc=1, device_id={"wall": w + 1}, device_id_type=MESH)

    def load(k):
        return pltpu.make_async_copy(
            noise.at[:, pl.ds(k * STEP, STEP)], stage.at[k], load_sem.at[k]
        )

    def start_load(k, _):
        load(k).start()
        return 0

    lax.fori_loop(0, chunks, start_load, 0)

    def to_above(k):
        return pltpu.make_async_remote_copy(
            src_ref=psi.at[k, 1], dst_ref=halo.at[k, 0],
            send_sem=wall_send.at[k, 0], recv_sem=wall_recv.at[k, 0],
            device_id={"wall": w + 1}, device_id_type=MESH,
        )

    def to_below(k):
        return pltpu.make_async_remote_copy(
            src_ref=psi.at[k, 0], dst_ref=halo.at[k, 1],
            send_sem=wall_send.at[k, 1], recv_sem=wall_recv.at[k, 1],
            device_id={"wall": w - 1}, device_id_type=MESH,
        )

    def to_right(k):
        return pltpu.make_async_remote_copy(
            src_ref=smooth.at[k], dst_ref=from_left.at[k],
            send_sem=span_send.at[k, 0], recv_sem=span_recv.at[k, 0],
            device_id={"span": right}, device_id_type=MESH,
        )

    def to_left(k):
        return pltpu.make_async_remote_copy(
            src_ref=smooth.at[k], dst_ref=from_right.at[k],
            send_sem=span_send.at[k, 1], recv_sem=span_recv.at[k, 1],
            device_id={"span": left}, device_id_type=MESH,
        )

    def convert(k):
        load(k).wait()
        for c in range(n_comp):
            for s in range(STEP):
                bits = stage[k, c, s].astype(jnp.float32)
                field = (math.sqrt(12.0) * ((bits + 0.5) * INV_RANGE - 0.5)).astype(jnp.bfloat16)
                at = (c * STEP + s) * n_cols
                psi[k, 0, at : at + n_cols, :] = field[:, :half]
                psi[k, 1, at : at + n_cols, :] = field[:, half:]

    def send_wall(k):
        @pl.when(above)
        def _():
            to_above(k).start()

        @pl.when(below)
        def _():
            to_below(k).start()

    convert(0)
    wall_bands(widths, raw, own_band, edge_band)
    span_band(z_band)
    carry[...] = jnp.zeros_like(carry)
    acc[...] = jnp.zeros_like(acc)

    @pl.when(jnp.logical_not(below))
    def _():
        def clear(k, _):
            halo[k, 0] = jnp.zeros(halo.shape[2:], halo.dtype)
            return 0

        lax.fori_loop(0, chunks, clear, 0)

    @pl.when(jnp.logical_not(above))
    def _():
        def clear(k, _):
            halo[k, 1] = jnp.zeros(halo.shape[2:], halo.dtype)
            return 0

        lax.fori_loop(0, chunks, clear, 0)

    pl.semaphore_wait(barrier, n_span - 1 + below.astype(jnp.int32) + above.astype(jnp.int32))

    send_wall(0)

    def convert_and_send(k, _):
        convert(k)
        send_wall(k)
        return 0

    lax.fori_loop(1, chunks, convert_and_send, 0)

    def wall_filter(k):
        @pl.when(below)
        def _():
            to_above(k).wait_recv()

        @pl.when(above)
        def _():
            to_below(k).wait_recv()

        own = jnp.concatenate([psi[k, 0], psi[k, 1]], axis=1)
        edge = jnp.concatenate([halo[k, 0], halo[k, 1]], axis=1)
        filtered = jnp.dot(own, own_band[...], preferred_element_type=jnp.float32) + jnp.dot(
            edge, edge_band[...], preferred_element_type=jnp.float32
        )
        smooth[k] = filtered.astype(jnp.bfloat16).reshape(smooth.shape[1:])
        to_right(k).start()
        to_left(k).start()

    def span_filter(k):
        to_right(k).wait_recv()
        to_left(k).wait_recv()
        for s in range(STEP):
            values = []
            fresh = jnp.where(k * STEP + s == 0, 1.0, FRESH)
            for c in range(n_comp):
                i = c * STEP + s
                window = jnp.concatenate([from_left[k, i], smooth[k, i], from_right[k, i]], axis=0)
                spanned = jnp.dot(z_band[...], window, preferred_element_type=jnp.float32)
                value = DECAY * carry[c] + fresh * spanned
                carry[c] = value
                fluct[c, k * STEP + s] = value
                values.append(value)
            for c in range(n_comp):
                acc[c] += jnp.sum(values[c].reshape(n_cols // 8, 8, n_rows), axis=0)
            for slot, (a, b) in enumerate(PAIRS):
                product = values[a] * values[b]
                acc[n_comp + slot] += jnp.sum(product.reshape(n_cols // 8, 8, n_rows), axis=0)

    def first_steps(k, _):
        wall_filter(k)
        return 0

    def middle_steps(k, _):
        wall_filter(k)
        span_filter(k - LAG)
        return 0

    def last_steps(k, _):
        span_filter(k)
        return 0

    lax.fori_loop(0, LAG, first_steps, 0)
    lax.fori_loop(LAG, chunks, middle_steps, 0)
    lax.fori_loop(chunks - LAG, chunks, last_steps, 0)

    sums[0] = jnp.concatenate(
        [jnp.sum(acc[...], axis=1), jnp.zeros((sums.shape[1] - acc.shape[0], n_rows), jnp.float32)],
        axis=0,
    )

    def share(i):
        return pltpu.make_async_remote_copy(
            src_ref=sums.at[0], dst_ref=sums.at[i],
            send_sem=sum_send.at[i], recv_sem=sum_recv.at[i],
            device_id={"span": lax.rem(p + i, n_span)}, device_id_type=MESH,
        )

    def start_share(i, _):
        share(i).start()
        return 0

    lax.fori_loop(1, n_span, start_share, 0)

    def collect(i, total):
        share(i).wait_recv()
        return total + sums[i]

    totals[...] = lax.fori_loop(1, n_span, collect, sums[0])

    def finish_share(i, _):
        share(i).wait_send()
        return 0

    lax.fori_loop(1, n_span, finish_share, 0)

    def finish_sends(k, _):
        @pl.when(above)
        def _():
            to_above(k).wait_send()

        @pl.when(below)
        def _():
            to_below(k).wait_send()

        to_right(k).wait_send()
        to_left(k).wait_send()
        return 0

    lax.fori_loop(0, chunks, finish_sends, 0)


def lund_transform(sample_covariance, target_factor_diagonal, target_factor_lower):
    cov_00 = sample_covariance[0] + SPREAD_FLOOR
    cov_10 = sample_covariance[1]
    cov_11 = sample_covariance[2] + SPREAD_FLOOR
    cov_20 = sample_covariance[3]
    cov_21 = sample_covariance[4]
    cov_22 = sample_covariance[5] + SPREAD_FLOOR
    chol_00 = jnp.sqrt(cov_00)
    chol_10 = cov_10 / chol_00
    chol_20 = cov_20 / chol_00
    chol_11 = jnp.sqrt(cov_11 - chol_10 * chol_10)
    chol_21 = (cov_21 - chol_20 * chol_10) / chol_11
    chol_22 = jnp.sqrt(cov_22 - chol_20 * chol_20 - chol_21 * chol_21)
    inv_00 = 1.0 / chol_00
    inv_11 = 1.0 / chol_11
    inv_22 = 1.0 / chol_22
    inv_10 = -chol_10 * inv_00 * inv_11
    inv_21 = -chol_21 * inv_11 * inv_22
    inv_20 = -(chol_20 * inv_00 + chol_21 * inv_10) * inv_22
    gain_00 = target_factor_diagonal[0] * inv_00
    gain_10 = target_factor_lower[0] * inv_00 + target_factor_diagonal[1] * inv_10
    gain_11 = target_factor_diagonal[1] * inv_11
    gain_20 = (
        target_factor_lower[1] * inv_00
        + target_factor_lower[2] * inv_10
        + target_factor_diagonal[2] * inv_20
    )
    gain_21 = target_factor_lower[2] * inv_11 + target_factor_diagonal[2] * inv_21
    gain_22 = target_factor_diagonal[2] * inv_22
    return (gain_00,), (gain_10, gain_11), (gain_20, gain_21, gain_22)


def scale_kernel(cell_count, fluct, totals, profile, diagonal, lower, out, gains):
    n_comp, n_step, n_cols, n_rows = fluct.shape

    @pl.when(pl.program_id(0) == 0)
    def _():
        row = [totals[i : i + 1, :] / cell_count for i in range(n_comp + len(PAIRS))]
        means = row[:n_comp]
        spread = [row[n_comp + slot] - means[a] * means[b] for slot, (a, b) in enumerate(PAIRS)]
        factors = lund_transform(
            spread,
            [diagonal[i : i + 1, :] for i in range(3)],
            [lower[i : i + 1, :] for i in range(3)],
        )
        flat = [g for line in factors for g in line]
        for i, value in enumerate(means + flat):
            gains[i] = jnp.broadcast_to(value, (8, n_rows))

    for s in range(n_step):
        centred = [
            fluct[c, s].reshape(n_cols // 8, 8, n_rows) - gains[c] for c in range(n_comp)
        ]
        at = n_comp
        for c in range(n_comp):
            value = profile[c : c + 1, :].reshape(1, 1, n_rows)
            for d in range(c + 1):
                value = value + gains[at] * centred[d]
                at += 1
            out[c, s] = value.reshape(n_cols, n_rows)


def shards(
    noise_bits, filter_widths, target_mean_profile, target_factor_diagonal, target_factor_lower
):
    n_comp, n_samples, n_cols, n_rows = noise_bits.shape
    n_wall, n_span = lax.axis_size("wall"), lax.axis_size("span")
    chunks = n_samples // STEP
    rows = n_comp * STEP * n_cols
    half = n_rows // 2
    bf16, f32 = jnp.bfloat16, jnp.float32
    dma = pltpu.SemaphoreType.DMA
    fluct, totals = pl.pallas_call(
        functools.partial(filter_kernel, n_wall, n_span),
        out_shape=(
            pltpu.VMEM((n_comp, n_samples, n_cols, n_rows), f32),
            pltpu.VMEM((16, n_rows), f32),
        ),
        in_specs=[
            pl.BlockSpec(memory_space=pltpu.HBM),
            pl.BlockSpec(memory_space=pltpu.VMEM),
        ],
        out_specs=(
            pl.BlockSpec(memory_space=pltpu.VMEM),
            pl.BlockSpec(memory_space=pltpu.VMEM),
        ),
        scratch_shapes=[
            pltpu.VMEM((chunks, n_comp, STEP, n_cols, n_rows), jnp.int32),
            pltpu.VMEM((chunks, 2, rows, half), bf16),
            pltpu.VMEM((chunks, 2, rows, half), bf16),
            pltpu.VMEM((chunks, n_comp * STEP, n_cols, n_rows), bf16),
            pltpu.VMEM((chunks, n_comp * STEP, n_cols, n_rows), bf16),
            pltpu.VMEM((chunks, n_comp * STEP, n_cols, n_rows), bf16),
            pltpu.VMEM((n_rows + 4 * WMAX, n_rows), f32),
            pltpu.VMEM((n_rows, n_rows), bf16),
            pltpu.VMEM((4 * WMAX, n_rows), bf16),
            pltpu.VMEM((n_cols, n_cols + 4 * SPANW), bf16),
            pltpu.VMEM((n_comp, n_cols, n_rows), f32),
            pltpu.VMEM((n_comp + len(PAIRS), 8, n_rows), f32),
            pltpu.VMEM((n_span, 16, n_rows), f32),
            dma((chunks,)),
            dma((chunks, 2)),
            dma((chunks, 2)),
            dma((chunks, 2)),
            dma((chunks, 2)),
            dma((n_span,)),
            dma((n_span,)),
        ],
        compiler_params=pltpu.CompilerParams(
            collective_id=0, has_side_effects=True, vmem_limit_bytes=40 * 1024 * 1024
        ),
        name="filters",
    )(
        pltpu.with_memory_space_constraint(noise_bits, pltpu.HBM), filter_widths.reshape(1, n_rows)
    )

    per_step = 2
    block = (n_comp, per_step, n_cols, n_rows)
    whole = lambda *shape: pl.BlockSpec(shape, lambda i: (0,) * len(shape))
    return pl.pallas_call(
        functools.partial(scale_kernel, float(n_samples * n_cols * n_span)),
        grid=(n_samples // per_step,),
        out_shape=jax.ShapeDtypeStruct(noise_bits.shape, f32),
        in_specs=[
            pl.BlockSpec(block, lambda i: (0, i, 0, 0)),
            whole(16, n_rows),
            whole(n_comp, n_rows),
            whole(n_comp, n_rows),
            whole(n_comp, n_rows),
        ],
        out_specs=pl.BlockSpec(block, lambda i: (0, i, 0, 0)),
        scratch_shapes=[pltpu.VMEM((n_comp + len(PAIRS), 8, n_rows), f32)],
        compiler_params=pltpu.CompilerParams(vmem_limit_bytes=16 * 1024 * 1024),
        name="rescale",
    )(fluct, totals, target_mean_profile, target_factor_diagonal, target_factor_lower)


def solution(mesh):
    placed = (
        P(None, None, "span", "wall"),
        P("wall"),
        P(None, "wall"),
        P(None, "wall"),
        P(None, "wall"),
    )
    return jax.shard_map(
        shards, mesh=mesh, in_specs=placed, out_specs=P(None, None, "span", "wall"), check_vma=False
    )
```

```python
import functools
import math

import jax
import jax.numpy as jnp
from jax import lax
from jax.experimental import pallas as pl
from jax.experimental.pallas import tpu as pltpu
from jax.sharding import PartitionSpec as P

WMAX = 64
SPANW = 32
TSCALE = 8
STEP = 2
LAG = 3

PAIRS = ((0, 0), (1, 0), (1, 1), (2, 0), (2, 1), (2, 2))
SPREAD_FLOOR = 0.25
INV_RANGE = 1.0 / 1073741824.0
DECAY = math.exp(-math.pi / (2.0 * TSCALE))
FRESH = math.sqrt(1.0 - DECAY * DECAY)
MESH = pl.DeviceIdType.MESH


def raw_taps(offsets, spread):
    inside = jnp.abs(offsets) <= 2.0 * spread
    safe_off = jnp.where(inside, offsets, 0.0)
    return jnp.where(
        inside, jnp.exp(-math.pi * safe_off * safe_off / (8.0 * spread * spread)), 0.0
    )


def wall_bands(widths_ref, raw_ref, own_ref, edge_ref):
    n_rows = widths_ref.shape[1]
    margin = 2 * WMAX
    block = 64
    count = (n_rows + 2 * margin) // block
    spread = widths_ref[...].astype(jnp.float32)

    def fill(i, total):
        at = pl.multiple_of(i * block, block)
        row = lax.broadcasted_iota(jnp.int32, (block, n_rows), 0) + i * block
        col = lax.broadcasted_iota(jnp.int32, (block, n_rows), 1)
        taps = raw_taps((row - margin - col).astype(jnp.float32), spread)
        raw_ref[pl.ds(at, block), :] = taps
        return total + jnp.sum(taps * taps, axis=0, keepdims=True)

    total = lax.fori_loop(0, count, fill, jnp.zeros((1, n_rows), jnp.float32))
    norm = jnp.sqrt(total)
    edge_ref[:margin, :] = (raw_ref[:margin, :] / norm).astype(jnp.bfloat16)
    own_ref[...] = (raw_ref[margin : margin + n_rows, :] / norm).astype(jnp.bfloat16)
    edge_ref[margin:, :] = (raw_ref[margin + n_rows :, :] / norm).astype(jnp.bfloat16)


def span_band(band_ref):
    n_cols, in_count = band_ref.shape
    margin = 2 * SPANW
    row = lax.broadcasted_iota(jnp.int32, (n_cols, in_count), 0)
    col = lax.broadcasted_iota(jnp.int32, (n_cols, in_count), 1)
    taps = raw_taps((col - margin - row).astype(jnp.float32), float(SPANW))
    norm = jnp.sqrt(jnp.sum(taps * taps, axis=1, keepdims=True))
    band_ref[...] = (taps / norm).astype(jnp.bfloat16)


def filter_kernel(
    n_wall, n_span, noise, widths, fluct, totals,
    stage, spread, psi, halo, smooth, sides, raw, own_band, edge_band, z_band, carry, acc, sums,
    load_sem, spread_sem, wall_send, wall_recv, span_send, span_recv, sum_send, sum_recv,
):
    n_comp, _, n_cols, n_rows = noise.shape
    chunks = stage.shape[0]
    half = n_rows // 2
    moments = acc.shape[0]
    w = lax.axis_index("wall")
    p = lax.axis_index("span")
    left, right = lax.rem(p + n_span - 1, n_span), lax.rem(p + 1, n_span)
    below, above = w > 0, w < n_wall - 1

    barrier = pltpu.get_barrier_semaphore()

    def greet(i, _):
        pl.semaphore_signal(
            barrier, inc=1, device_id={"span": lax.rem(p + i, n_span)}, device_id_type=MESH
        )
        return 0

    lax.fori_loop(1, n_span, greet, 0)

    @pl.when(below)
    def _():
        pl.semaphore_signal(barrier, inc=1, device_id={"wall": w - 1}, device_id_type=MESH)

    @pl.when(above)
    def _():
        pl.semaphore_signal(barrier, inc=1, device_id={"wall": w + 1}, device_id_type=MESH)

    def load(k):
        return pltpu.make_async_copy(
            noise.at[:, pl.ds(k * STEP, STEP)], stage.at[k], load_sem.at[k]
        )

    def start_load(k, _):
        load(k).start()
        return 0

    load_spread = pltpu.make_async_copy(widths, spread, spread_sem)
    load(0).start()
    load_spread.start()
    lax.fori_loop(1, chunks, start_load, 0)

    def to_above(k):
        return pltpu.make_async_remote_copy(
            src_ref=psi.at[k, 1], dst_ref=halo.at[k, 0],
            send_sem=wall_send.at[0], recv_sem=wall_recv.at[k],
            device_id={"wall": w + 1}, device_id_type=MESH,
        )

    def to_below(k):
        return pltpu.make_async_remote_copy(
            src_ref=psi.at[k, 0], dst_ref=halo.at[k, 1],
            send_sem=wall_send.at[1], recv_sem=wall_recv.at[k],
            device_id={"wall": w - 1}, device_id_type=MESH,
        )

    def to_right(k):
        return pltpu.make_async_remote_copy(
            src_ref=smooth.at[k], dst_ref=sides.at[k, 0],
            send_sem=span_send.at[0], recv_sem=span_recv.at[k],
            device_id={"span": right}, device_id_type=MESH,
        )

    def to_left(k):
        return pltpu.make_async_remote_copy(
            src_ref=smooth.at[k], dst_ref=sides.at[k, 1],
            send_sem=span_send.at[1], recv_sem=span_recv.at[k],
            device_id={"span": left}, device_id_type=MESH,
        )

    def landed(ref, sem):
        pltpu.make_async_copy(ref, ref, sem).wait()

    def convert(k):
        load(k).wait()
        for c in range(n_comp):
            for s in range(STEP):
                bits = stage[k, c, s].astype(jnp.float32)
                field = (math.sqrt(12.0) * ((bits + 0.5) * INV_RANGE - 0.5)).astype(jnp.bfloat16)
                at = (c * STEP + s) * n_cols
                psi[k, 0, at : at + n_cols, :] = field[:, :half]
                psi[k, 1, at : at + n_cols, :] = field[:, half:]

    def send_wall(k):
        @pl.when(above)
        def _():
            to_above(k).start()

        @pl.when(below)
        def _():
            to_below(k).start()

    with jax.named_scope("first_convert"):
        convert(0)
    with jax.named_scope("bands"):
        load_spread.wait()
        wall_bands(spread, raw, own_band, edge_band)
        span_band(z_band)
    carry[...] = jnp.zeros_like(carry)
    acc[...] = jnp.zeros_like(acc)

    @pl.when(jnp.logical_not(below))
    def _():
        def clear(k, _):
            halo[k, 0] = jnp.zeros(halo.shape[2:], halo.dtype)
            return 0

        lax.fori_loop(0, chunks, clear, 0)

    @pl.when(jnp.logical_not(above))
    def _():
        def clear(k, _):
            halo[k, 1] = jnp.zeros(halo.shape[2:], halo.dtype)
            return 0

        lax.fori_loop(0, chunks, clear, 0)

    with jax.named_scope("greeted"):
        pl.semaphore_wait(barrier, n_span - 1 + below.astype(jnp.int32) + above.astype(jnp.int32))

    send_wall(0)

    def convert_and_send(k, _):
        convert(k)
        send_wall(k)
        return 0

    lax.fori_loop(1, chunks, convert_and_send, 0)

    def wall_arrived(k):
        @pl.when(jnp.logical_and(below, above))
        def _():
            landed(halo.at[k], wall_recv.at[k])

        @pl.when(jnp.logical_not(below))
        def _():
            landed(halo.at[k, 1], wall_recv.at[k])

        @pl.when(jnp.logical_not(above))
        def _():
            landed(halo.at[k, 0], wall_recv.at[k])

    def wall_filter(k):
        with jax.named_scope("wall_wait"):
            wall_arrived(k)
        own = jnp.concatenate([psi[k, 0], psi[k, 1]], axis=1)
        edge = jnp.concatenate([halo[k, 0], halo[k, 1]], axis=1)
        filtered = jnp.dot(own, own_band[...], preferred_element_type=jnp.float32) + jnp.dot(
            edge, edge_band[...], preferred_element_type=jnp.float32
        )
        smooth[k] = filtered.astype(jnp.bfloat16).reshape(smooth.shape[1:])
        to_right(k).start()
        to_left(k).start()

    def span_filter(k):
        with jax.named_scope("span_wait"):
            landed(sides.at[k], span_recv.at[k])
        for s in range(STEP):
            values = []
            fresh = jnp.where(k * STEP + s == 0, 1.0, FRESH)
            for c in range(n_comp):
                i = c * STEP + s
                window = jnp.concatenate([sides[k, 0, i], smooth[k, i], sides[k, 1, i]], axis=0)
                spanned = jnp.dot(z_band[...], window, preferred_element_type=jnp.float32)
                value = DECAY * carry[c] + fresh * spanned
                carry[c] = value
                fluct[c, k * STEP + s] = value
                values.append(value)
            for c in range(n_comp):
                acc[c] += jnp.sum(values[c].reshape(n_cols // 8, 8, n_rows), axis=0)
            for slot, (a, b) in enumerate(PAIRS):
                product = values[a] * values[b]
                acc[n_comp + slot] += jnp.sum(product.reshape(n_cols // 8, 8, n_rows), axis=0)

    def first_steps(k, _):
        wall_filter(k)
        return 0

    def middle_steps(k, _):
        wall_filter(k)
        span_filter(k - LAG)
        return 0

    def last_steps(k, _):
        span_filter(k)
        return 0

    lax.fori_loop(0, LAG, first_steps, 0)
    lax.fori_loop(LAG, chunks, middle_steps, 0)
    lax.fori_loop(chunks - LAG, chunks, last_steps, 0)

    for m in range(moments):
        sums[0, m] = jnp.sum(acc[m], axis=0, keepdims=True)

    def share(i, _):
        pltpu.make_async_remote_copy(
            src_ref=sums.at[0], dst_ref=sums.at[i],
            send_sem=sum_send, recv_sem=sum_recv,
            device_id={"span": lax.rem(p + i, n_span)}, device_id_type=MESH,
        ).start()
        return 0

    lax.fori_loop(1, n_span, share, 0)

    with jax.named_scope("send_ends"):

        @pl.when(above)
        def _():
            landed(psi.at[:, 1], wall_send.at[0])

        @pl.when(below)
        def _():
            landed(psi.at[:, 0], wall_send.at[1])

        landed(smooth, span_send.at[0])
        landed(smooth, span_send.at[1])

    others = sums.at[pl.ds(1, n_span - 1)]
    with jax.named_scope("sums_wait"):
        landed(others, sum_recv)

    def collect(i, total):
        return total + sums[i]

    totals[...] = lax.fori_loop(1, n_span, collect, sums[0])
    with jax.named_scope("share_ends"):
        landed(others, sum_send)


def lund_transform(sample_covariance, target_factor_diagonal, target_factor_lower):
    cov_00 = sample_covariance[0] + SPREAD_FLOOR
    cov_10 = sample_covariance[1]
    cov_11 = sample_covariance[2] + SPREAD_FLOOR
    cov_20 = sample_covariance[3]
    cov_21 = sample_covariance[4]
    cov_22 = sample_covariance[5] + SPREAD_FLOOR
    chol_00 = jnp.sqrt(cov_00)
    chol_10 = cov_10 / chol_00
    chol_20 = cov_20 / chol_00
    chol_11 = jnp.sqrt(cov_11 - chol_10 * chol_10)
    chol_21 = (cov_21 - chol_20 * chol_10) / chol_11
    chol_22 = jnp.sqrt(cov_22 - chol_20 * chol_20 - chol_21 * chol_21)
    inv_00 = 1.0 / chol_00
    inv_11 = 1.0 / chol_11
    inv_22 = 1.0 / chol_22
    inv_10 = -chol_10 * inv_00 * inv_11
    inv_21 = -chol_21 * inv_11 * inv_22
    inv_20 = -(chol_20 * inv_00 + chol_21 * inv_10) * inv_22
    gain_00 = target_factor_diagonal[0] * inv_00
    gain_10 = target_factor_lower[0] * inv_00 + target_factor_diagonal[1] * inv_10
    gain_11 = target_factor_diagonal[1] * inv_11
    gain_20 = (
        target_factor_lower[1] * inv_00
        + target_factor_lower[2] * inv_10
        + target_factor_diagonal[2] * inv_20
    )
    gain_21 = target_factor_lower[2] * inv_11 + target_factor_diagonal[2] * inv_21
    gain_22 = target_factor_diagonal[2] * inv_22
    return (gain_00,), (gain_10, gain_11), (gain_20, gain_21, gain_22)


def scale_kernel(cell_count, fluct, totals, profile, diagonal, lower, out, ready, sem):
    n_comp, n_samples, n_cols, n_rows = fluct.shape
    row = [totals[i] / cell_count for i in range(n_comp + len(PAIRS))]
    means = row[:n_comp]
    spread = [row[n_comp + slot] - means[a] * means[b] for slot, (a, b) in enumerate(PAIRS)]
    factors = lund_transform(
        spread,
        [diagonal[i : i + 1, :] for i in range(3)],
        [lower[i : i + 1, :] for i in range(3)],
    )

    def one_sample(s, _):
        centred = [fluct[c, s] - means[c] for c in range(n_comp)]
        for c in range(n_comp):
            value = profile[c : c + 1, :]
            for d in range(c + 1):
                value = value + factors[c][d] * centred[d]
            ready[c, s] = value
        pltpu.make_async_copy(ready.at[:, s], out.at[:, s], sem).start()
        return 0

    lax.fori_loop(0, n_samples, one_sample, 0)
    pltpu.make_async_copy(ready, out, sem).wait()


def shards(
    noise_bits, filter_widths, target_mean_profile, target_factor_diagonal, target_factor_lower
):
    n_comp, n_samples, n_cols, n_rows = noise_bits.shape
    n_wall, n_span = lax.axis_size("wall"), lax.axis_size("span")
    chunks = n_samples // STEP
    rows = n_comp * STEP * n_cols
    half = n_rows // 2
    moments = n_comp + len(PAIRS)
    bf16, f32 = jnp.bfloat16, jnp.float32
    dma = pltpu.SemaphoreType.DMA
    fluct, totals = pl.pallas_call(
        functools.partial(filter_kernel, n_wall, n_span),
        out_shape=(
            pltpu.VMEM((n_comp, n_samples, n_cols, n_rows), f32),
            pltpu.VMEM((moments, 1, n_rows), f32),
        ),
        in_specs=[
            pl.BlockSpec(memory_space=pltpu.HBM),
            pl.BlockSpec(memory_space=pltpu.HBM),
        ],
        out_specs=(
            pl.BlockSpec(memory_space=pltpu.VMEM),
            pl.BlockSpec(memory_space=pltpu.VMEM),
        ),
        scratch_shapes=[
            pltpu.VMEM((chunks, n_comp, STEP, n_cols, n_rows), jnp.int32),
            pltpu.VMEM((1, n_rows), jnp.int32),
            pltpu.VMEM((chunks, 2, rows, half), bf16),
            pltpu.VMEM((chunks, 2, rows, half), bf16),
            pltpu.VMEM((chunks, n_comp * STEP, n_cols, n_rows), bf16),
            pltpu.VMEM((chunks, 2, n_comp * STEP, n_cols, n_rows), bf16),
            pltpu.VMEM((n_rows + 4 * WMAX, n_rows), f32),
            pltpu.VMEM((n_rows, n_rows), bf16),
            pltpu.VMEM((4 * WMAX, n_rows), bf16),
            pltpu.VMEM((n_cols, n_cols + 4 * SPANW), bf16),
            pltpu.VMEM((n_comp, n_cols, n_rows), f32),
            pltpu.VMEM((moments, 8, n_rows), f32),
            pltpu.VMEM((n_span, moments, 1, n_rows), f32),
            dma((chunks,)),
            dma,
            dma((2,)),
            dma((chunks,)),
            dma((2,)),
            dma((chunks,)),
            dma,
            dma,
        ],
        compiler_params=pltpu.CompilerParams(
            collective_id=0, has_side_effects=True, vmem_limit_bytes=40 * 1024 * 1024
        ),
        name="filters",
    )(
        pltpu.with_memory_space_constraint(noise_bits, pltpu.HBM),
        pltpu.with_memory_space_constraint(filter_widths.reshape(1, n_rows), pltpu.HBM),
    )

    in_vmem = pl.BlockSpec(memory_space=pltpu.VMEM)
    return pl.pallas_call(
        functools.partial(scale_kernel, float(n_samples * n_cols * n_span)),
        out_shape=pltpu.HBM(noise_bits.shape, f32),
        in_specs=[in_vmem] * 5,
        out_specs=pl.BlockSpec(memory_space=pltpu.HBM),
        scratch_shapes=[pltpu.VMEM(noise_bits.shape, f32), dma],
        compiler_params=pltpu.CompilerParams(vmem_limit_bytes=16 * 1024 * 1024),
        name="rescale",
    )(fluct, totals, target_mean_profile, target_factor_diagonal, target_factor_lower)


def solution(mesh):
    placed = (
        P(None, None, "span", "wall"),
        P("wall"),
        P(None, "wall"),
        P(None, "wall"),
        P(None, "wall"),
    )
    return jax.shard_map(
        shards, mesh=mesh, in_specs=placed, out_specs=P(None, None, "span", "wall"), check_vma=False
    )
```

```python
import functools
import math

import jax
import jax.numpy as jnp
from jax import lax
from jax.experimental import pallas as pl
from jax.experimental.pallas import tpu as pltpu
from jax.sharding import PartitionSpec as P

WMAX = 64
SPANW = 32
TSCALE = 8
STEP = 2
LAG = 4
FIRST = 3

PAIRS = ((0, 0), (1, 0), (1, 1), (2, 0), (2, 1), (2, 2))
SPREAD_FLOOR = 0.25
INV_RANGE = 1.0 / 1073741824.0
DECAY = math.exp(-math.pi / (2.0 * TSCALE))
FRESH = math.sqrt(1.0 - DECAY * DECAY)
MESH = pl.DeviceIdType.MESH


def raw_taps(offsets, spread):
    inside = jnp.abs(offsets) <= 2.0 * spread
    safe_off = jnp.where(inside, offsets, 0.0)
    return jnp.where(
        inside, jnp.exp(-math.pi * safe_off * safe_off / (8.0 * spread * spread)), 0.0
    )


def wall_bands(widths_ref, raw_ref, own_ref, edge_ref):
    n_rows = widths_ref.shape[1]
    margin = 2 * WMAX
    block = 64
    count = (n_rows + 2 * margin) // block
    spread = widths_ref[...].astype(jnp.float32)

    def fill(i, total):
        at = pl.multiple_of(i * block, block)
        row = lax.broadcasted_iota(jnp.int32, (block, n_rows), 0) + i * block
        col = lax.broadcasted_iota(jnp.int32, (block, n_rows), 1)
        taps = raw_taps((row - margin - col).astype(jnp.float32), spread)
        raw_ref[pl.ds(at, block), :] = taps
        return total + jnp.sum(taps * taps, axis=0, keepdims=True)

    total = lax.fori_loop(0, count, fill, jnp.zeros((1, n_rows), jnp.float32))
    norm = jnp.sqrt(total)
    edge_ref[:margin, :] = (raw_ref[:margin, :] / norm).astype(jnp.bfloat16)
    own_ref[...] = (raw_ref[margin : margin + n_rows, :] / norm).astype(jnp.bfloat16)
    edge_ref[margin:, :] = (raw_ref[margin + n_rows :, :] / norm).astype(jnp.bfloat16)


def span_band(band_ref):
    n_cols, in_count = band_ref.shape
    margin = 2 * SPANW
    row = lax.broadcasted_iota(jnp.int32, (n_cols, in_count), 0)
    col = lax.broadcasted_iota(jnp.int32, (n_cols, in_count), 1)
    taps = raw_taps((col - margin - row).astype(jnp.float32), float(SPANW))
    norm = jnp.sqrt(jnp.sum(taps * taps, axis=1, keepdims=True))
    band_ref[...] = (taps / norm).astype(jnp.bfloat16)


def filter_kernel(
    n_wall, n_span, noise, widths, fluct, totals,
    stage, spread, psi, halo, smooth, sides, raw, own_band, edge_band, z_band, carry, acc, sums,
    load_sem, spread_sem, meet, wall_send, wall_recv, span_send, span_recv, sum_send, sum_recv,
):
    n_comp, _, n_cols, n_rows = noise.shape
    chunks = stage.shape[0]
    half = n_rows // 2
    moments = acc.shape[0]
    w = lax.axis_index("wall")
    p = lax.axis_index("span")
    left, right = lax.rem(p + n_span - 1, n_span), lax.rem(p + 1, n_span)
    below, above = w > 0, w < n_wall - 1

    barrier = pltpu.get_barrier_semaphore()

    def signal(where, **device):
        pl.semaphore_signal(where, inc=1, device_id=device, device_id_type=MESH)

    signal(barrier, span=left)
    signal(barrier, span=right)

    @pl.when(below)
    def _():
        signal(barrier, wall=w - 1)

    @pl.when(above)
    def _():
        signal(barrier, wall=w + 1)

    rounds = (n_span // 2).bit_length() - 1

    def reach(r):
        if r < rounds:
            signal(meet.at[r], span=lax.rem(p + 2**r, n_span))
            signal(meet.at[r], span=lax.rem(p + n_span - 2**r, n_span))

    def reached(r):
        if r < rounds:
            pl.semaphore_wait(meet.at[r], 2)

    n_wall_first = chunks - FIRST
    order = [k for i in range(FIRST) for k in (n_wall_first + i, i)]
    late = n_wall_first - FIRST

    def load(k, sem):
        return pltpu.make_async_copy(noise.at[:, pl.ds(k * STEP, STEP)], stage.at[k], load_sem.at[sem])

    def start_load(k, _):
        load(k, len(order)).start()
        return 0

    load_spread = pltpu.make_async_copy(widths, spread, spread_sem)
    for sem, k in enumerate(order):
        load(k, sem).start()
    load_spread.start()
    lax.fori_loop(FIRST, n_wall_first, start_load, 0)

    def to_above(k):
        return pltpu.make_async_remote_copy(
            src_ref=psi.at[k, 1], dst_ref=halo.at[k, 0],
            send_sem=wall_send.at[0], recv_sem=wall_recv.at[k],
            device_id={"wall": w + 1}, device_id_type=MESH,
        )

    def to_below(k):
        return pltpu.make_async_remote_copy(
            src_ref=psi.at[k, 0], dst_ref=halo.at[k, 1],
            send_sem=wall_send.at[1], recv_sem=wall_recv.at[k],
            device_id={"wall": w - 1}, device_id_type=MESH,
        )

    def to_right(k):
        return pltpu.make_async_remote_copy(
            src_ref=smooth.at[k], dst_ref=sides.at[k, 0],
            send_sem=span_send.at[0], recv_sem=span_recv.at[k],
            device_id={"span": right}, device_id_type=MESH,
        )

    def to_left(k):
        return pltpu.make_async_remote_copy(
            src_ref=smooth.at[k], dst_ref=sides.at[k, 1],
            send_sem=span_send.at[1], recv_sem=span_recv.at[k],
            device_id={"span": left}, device_id_type=MESH,
        )

    def landed(ref, sem):
        pltpu.make_async_copy(ref, ref, sem).wait()

    def convert(k, span_first):
        for c in range(n_comp):
            for s in range(STEP):
                bits = stage[k, c, s].astype(jnp.float32)
                field = (math.sqrt(12.0) * ((bits + 0.5) * INV_RANGE - 0.5)).astype(jnp.bfloat16)
                if span_first:
                    smooth[k, c * STEP + s] = field
                else:
                    at = (c * STEP + s) * n_cols
                    psi[k, 0, at : at + n_cols, :] = field[:, :half]
                    psi[k, 1, at : at + n_cols, :] = field[:, half:]

    def send_wall(k):
        @pl.when(above)
        def _():
            to_above(k).start()

        @pl.when(below)
        def _():
            to_below(k).start()

    def send_span(k):
        to_right(k).start()
        to_left(k).start()

    for sem, k in enumerate(order):
        with jax.named_scope("early_convert"):
            load(k, sem).wait()
            convert(k, k >= n_wall_first)
        if k == order[0]:
            with jax.named_scope("greeted"):
                pl.semaphore_wait(barrier, 2 + below.astype(jnp.int32) + above.astype(jnp.int32))
        if k >= n_wall_first:
            send_span(k)
        else:
            send_wall(k)

    def convert_and_send(k, _):
        convert(k, False)
        send_wall(k)
        return 0

    reach(0)
    with jax.named_scope("converts"):
        landed(stage.at[pl.ds(FIRST, late)], load_sem.at[len(order)])
        lax.fori_loop(FIRST, n_wall_first, convert_and_send, 0)
    with jax.named_scope("bands"):
        load_spread.wait()
        wall_bands(spread, raw, own_band, edge_band)
        span_band(z_band)
    carry[...] = jnp.zeros_like(carry)
    acc[...] = jnp.zeros_like(acc)

    @pl.when(jnp.logical_not(below))
    def _():
        def clear(k, _):
            halo[k, 0] = jnp.zeros(halo.shape[2:], halo.dtype)
            return 0

        lax.fori_loop(0, chunks, clear, 0)

    @pl.when(jnp.logical_not(above))
    def _():
        def clear(k, _):
            halo[k, 1] = jnp.zeros(halo.shape[2:], halo.dtype)
            return 0

        lax.fori_loop(0, chunks, clear, 0)

    def wall_arrived(k):
        @pl.when(jnp.logical_and(below, above))
        def _():
            landed(halo.at[k], wall_recv.at[k])

        @pl.when(jnp.logical_not(below))
        def _():
            landed(halo.at[k, 1], wall_recv.at[k])

        @pl.when(jnp.logical_not(above))
        def _():
            landed(halo.at[k, 0], wall_recv.at[k])

    def wall_sum(k):
        with jax.named_scope("wall_wait"):
            wall_arrived(k)
        own = jnp.concatenate([psi[k, 0], psi[k, 1]], axis=1)
        edge = jnp.concatenate([halo[k, 0], halo[k, 1]], axis=1)
        total = jnp.dot(own, own_band[...], preferred_element_type=jnp.float32) + jnp.dot(
            edge, edge_band[...], preferred_element_type=jnp.float32
        )
        return total.reshape(n_comp * STEP, n_cols, n_rows)

    def span_arrived(k):
        with jax.named_scope("span_wait"):
            landed(sides.at[k], span_recv.at[k])

    def span_sum(k, i):
        window = jnp.concatenate([sides[k, 0, i], smooth[k, i], sides[k, 1, i]], axis=0)
        return jnp.dot(z_band[...], window, preferred_element_type=jnp.float32)

    def wall_filter(k):
        smooth[k] = wall_sum(k).astype(jnp.bfloat16)
        send_span(k)

    def span_filter_first(k):
        span_arrived(k)
        for i in range(n_comp * STEP):
            field = span_sum(k, i).astype(jnp.bfloat16)
            psi[k, 0, i * n_cols : (i + 1) * n_cols, :] = field[:, :half]
            psi[k, 1, i * n_cols : (i + 1) * n_cols, :] = field[:, half:]
        send_wall(k)

    def advance(k, filtered):
        for s in range(STEP):
            fresh = jnp.where(k * STEP + s == 0, 1.0, FRESH)
            values = []
            for c in range(n_comp):
                value = DECAY * carry[c] + fresh * filtered(c, s)
                carry[c] = value
                fluct[c, k * STEP + s] = value
                values.append(value)
            for c in range(n_comp):
                acc[c] += jnp.sum(values[c].reshape(n_cols // 8, 8, n_rows), axis=0)
            for slot, (a, b) in enumerate(PAIRS):
                product = values[a] * values[b]
                acc[n_comp + slot] += jnp.sum(product.reshape(n_cols // 8, 8, n_rows), axis=0)

    def span_filter(k):
        span_arrived(k)
        advance(k, lambda c, s: span_sum(k, c * STEP + s))

    def wall_filter_last(k):
        fields = wall_sum(k)
        for c in range(n_comp):
            for s in range(STEP):
                fluct[c, k * STEP + s] = fields[c * STEP + s]

    def middle_steps(k, _):
        wall_filter(k)
        span_filter(k - LAG)
        return 0

    def last_steps(k, _):
        span_filter(k)
        return 0

    for k in range(LAG):
        wall_filter(k)
        if k < FIRST:
            span_filter_first(n_wall_first + k)
        reached(k)
        reach(k + 1)
    lax.fori_loop(LAG, n_wall_first, middle_steps, 0)
    for r in range(LAG, rounds):
        reached(r)
        reach(r + 1)
    lax.fori_loop(n_wall_first - LAG, n_wall_first - 1, last_steps, 0)
    for k in range(n_wall_first, chunks):
        wall_filter_last(k)
    span_filter(n_wall_first - 1)
    for k in range(n_wall_first, chunks):
        advance(k, lambda c, s: fluct[c, k * STEP + s])
    for m in range(moments):
        sums[0, m] = jnp.sum(acc[m], axis=0, keepdims=True)

    n_y = min(4, n_span // 2)
    n_x = n_span // (2 * n_y)
    x, y, core = p // (2 * n_y), lax.rem(p // 2, n_y), lax.rem(p, 2)

    def hops(step):
        return min(step[0], n_x - step[0]) + min(step[1], n_y - step[1])

    steps = [(dx, dy, dc) for dx in range(n_x) for dy in range(n_y) for dc in range(2)]
    steps.sort(key=hops)
    with jax.named_scope("share"):
        for i in reversed(range(1, n_span)):
            dx, dy, dc = steps[i]
            there = (lax.rem(x + dx, n_x) * n_y + lax.rem(y + dy, n_y)) * 2 + lax.rem(core + dc, 2)
            pltpu.make_async_remote_copy(
                src_ref=sums.at[0], dst_ref=sums.at[i],
                send_sem=sum_send, recv_sem=sum_recv,
                device_id={"span": there}, device_id_type=MESH,
            ).start()

    with jax.named_scope("send_ends"):

        @pl.when(above)
        def _():
            landed(psi.at[:, 1], wall_send.at[0])

        @pl.when(below)
        def _():
            landed(psi.at[:, 0], wall_send.at[1])

        landed(smooth, span_send.at[0])
        landed(smooth, span_send.at[1])

    others = sums.at[pl.ds(1, n_span - 1)]
    with jax.named_scope("sums_wait"):
        landed(others, sum_recv)

    def collect(i, total):
        return total + sums[i]

    totals[...] = lax.fori_loop(1, n_span, collect, sums[0])
    with jax.named_scope("share_ends"):
        landed(others, sum_send)


def lund_transform(sample_covariance, target_factor_diagonal, target_factor_lower):
    cov_00 = sample_covariance[0] + SPREAD_FLOOR
    cov_10 = sample_covariance[1]
    cov_11 = sample_covariance[2] + SPREAD_FLOOR
    cov_20 = sample_covariance[3]
    cov_21 = sample_covariance[4]
    cov_22 = sample_covariance[5] + SPREAD_FLOOR
    chol_00 = jnp.sqrt(cov_00)
    chol_10 = cov_10 / chol_00
    chol_20 = cov_20 / chol_00
    chol_11 = jnp.sqrt(cov_11 - chol_10 * chol_10)
    chol_21 = (cov_21 - chol_20 * chol_10) / chol_11
    chol_22 = jnp.sqrt(cov_22 - chol_20 * chol_20 - chol_21 * chol_21)
    inv_00 = 1.0 / chol_00
    inv_11 = 1.0 / chol_11
    inv_22 = 1.0 / chol_22
    inv_10 = -chol_10 * inv_00 * inv_11
    inv_21 = -chol_21 * inv_11 * inv_22
    inv_20 = -(chol_20 * inv_00 + chol_21 * inv_10) * inv_22
    gain_00 = target_factor_diagonal[0] * inv_00
    gain_10 = target_factor_lower[0] * inv_00 + target_factor_diagonal[1] * inv_10
    gain_11 = target_factor_diagonal[1] * inv_11
    gain_20 = (
        target_factor_lower[1] * inv_00
        + target_factor_lower[2] * inv_10
        + target_factor_diagonal[2] * inv_20
    )
    gain_21 = target_factor_lower[2] * inv_11 + target_factor_diagonal[2] * inv_21
    gain_22 = target_factor_diagonal[2] * inv_22
    return (gain_00,), (gain_10, gain_11), (gain_20, gain_21, gain_22)


def scale_kernel(cell_count, fluct, totals, profile, diagonal, lower, out, ready, sem):
    n_comp, n_samples, n_cols, n_rows = fluct.shape
    row = [totals[i] / cell_count for i in range(n_comp + len(PAIRS))]
    means = row[:n_comp]
    spread = [row[n_comp + slot] - means[a] * means[b] for slot, (a, b) in enumerate(PAIRS)]
    factors = lund_transform(
        spread,
        [diagonal[i : i + 1, :] for i in range(3)],
        [lower[i : i + 1, :] for i in range(3)],
    )

    def one_sample(s, _):
        centred = [fluct[c, s] - means[c] for c in range(n_comp)]
        for c in range(n_comp):
            value = profile[c : c + 1, :]
            for d in range(c + 1):
                value = value + factors[c][d] * centred[d]
            ready[c, s] = value
        pltpu.make_async_copy(ready.at[:, s], out.at[:, s], sem).start()
        return 0

    lax.fori_loop(0, n_samples, one_sample, 0)
    pltpu.make_async_copy(ready, out, sem).wait()


def shards(
    noise_bits, filter_widths, target_mean_profile, target_factor_diagonal, target_factor_lower
):
    n_comp, n_samples, n_cols, n_rows = noise_bits.shape
    n_wall, n_span = lax.axis_size("wall"), lax.axis_size("span")
    chunks = n_samples // STEP
    rows = n_comp * STEP * n_cols
    half = n_rows // 2
    moments = n_comp + len(PAIRS)
    bf16, f32 = jnp.bfloat16, jnp.float32
    dma = pltpu.SemaphoreType.DMA
    fluct, totals = pl.pallas_call(
        functools.partial(filter_kernel, n_wall, n_span),
        out_shape=(
            pltpu.VMEM((n_comp, n_samples, n_cols, n_rows), f32),
            pltpu.VMEM((moments, 1, n_rows), f32),
        ),
        in_specs=[
            pl.BlockSpec(memory_space=pltpu.HBM),
            pl.BlockSpec(memory_space=pltpu.HBM),
        ],
        out_specs=(
            pl.BlockSpec(memory_space=pltpu.VMEM),
            pl.BlockSpec(memory_space=pltpu.VMEM),
        ),
        scratch_shapes=[
            pltpu.VMEM((chunks, n_comp, STEP, n_cols, n_rows), jnp.int32),
            pltpu.VMEM((1, n_rows), jnp.int32),
            pltpu.VMEM((chunks, 2, rows, half), bf16),
            pltpu.VMEM((chunks, 2, rows, half), bf16),
            pltpu.VMEM((chunks, n_comp * STEP, n_cols, n_rows), bf16),
            pltpu.VMEM((chunks, 2, n_comp * STEP, n_cols, n_rows), bf16),
            pltpu.VMEM((n_rows + 4 * WMAX, n_rows), f32),
            pltpu.VMEM((n_rows, n_rows), bf16),
            pltpu.VMEM((4 * WMAX, n_rows), bf16),
            pltpu.VMEM((n_cols, n_cols + 4 * SPANW), bf16),
            pltpu.VMEM((n_comp, n_cols, n_rows), f32),
            pltpu.VMEM((moments, 8, n_rows), f32),
            pltpu.VMEM((n_span, moments, 1, n_rows), f32),
            dma((2 * FIRST + 1,)),
            dma,
            pltpu.SemaphoreType.REGULAR((max(1, (n_span // 2).bit_length() - 1),)),
            dma((2,)),
            dma((chunks,)),
            dma((2,)),
            dma((chunks,)),
            dma,
            dma,
        ],
        compiler_params=pltpu.CompilerParams(
            collective_id=0, has_side_effects=True, vmem_limit_bytes=40 * 1024 * 1024
        ),
        name="filters",
    )(
        pltpu.with_memory_space_constraint(noise_bits, pltpu.HBM),
        pltpu.with_memory_space_constraint(filter_widths.reshape(1, n_rows), pltpu.HBM),
    )

    in_vmem = pl.BlockSpec(memory_space=pltpu.VMEM)
    return pl.pallas_call(
        functools.partial(scale_kernel, float(n_samples * n_cols * n_span)),
        out_shape=pltpu.HBM(noise_bits.shape, f32),
        in_specs=[in_vmem] * 5,
        out_specs=pl.BlockSpec(memory_space=pltpu.HBM),
        scratch_shapes=[pltpu.VMEM(noise_bits.shape, f32), dma],
        compiler_params=pltpu.CompilerParams(vmem_limit_bytes=16 * 1024 * 1024),
        name="rescale",
    )(fluct, totals, target_mean_profile, target_factor_diagonal, target_factor_lower)


def solution(mesh):
    placed = (
        P(None, None, "span", "wall"),
        P("wall"),
        P(None, "wall"),
        P(None, "wall"),
        P(None, "wall"),
    )
    return jax.shard_map(
        shards, mesh=mesh, in_specs=placed, out_specs=P(None, None, "span", "wall"), check_vma=False
    )
```

```python
import functools
import math

import jax
import jax.numpy as jnp
from jax import lax
from jax.experimental import pallas as pl
from jax.experimental.pallas import tpu as pltpu
from jax.sharding import PartitionSpec as P

WMAX = 64
SPANW = 32
TSCALE = 8
STEP = 2
LAG = 5
FIRST = 4

PAIRS = ((0, 0), (1, 0), (1, 1), (2, 0), (2, 1), (2, 2))
SPREAD_FLOOR = 0.25
INV_RANGE = 1.0 / 1073741824.0
DECAY = math.exp(-math.pi / (2.0 * TSCALE))
FRESH = math.sqrt(1.0 - DECAY * DECAY)
MESH = pl.DeviceIdType.MESH


def raw_taps(offsets, spread):
    inside = jnp.abs(offsets) <= 2.0 * spread
    safe_off = jnp.where(inside, offsets, 0.0)
    return jnp.where(
        inside, jnp.exp(-math.pi * safe_off * safe_off / (8.0 * spread * spread)), 0.0
    )


def wall_bands(widths_ref, raw_ref, own_ref, edge_ref):
    n_rows = widths_ref.shape[1]
    margin = 2 * WMAX
    block = 64
    count = (n_rows + 2 * margin) // block
    spread = widths_ref[...].astype(jnp.float32)

    def fill(i, total):
        at = pl.multiple_of(i * block, block)
        row = lax.broadcasted_iota(jnp.int32, (block, n_rows), 0) + i * block
        col = lax.broadcasted_iota(jnp.int32, (block, n_rows), 1)
        taps = raw_taps((row - margin - col).astype(jnp.float32), spread)
        raw_ref[pl.ds(at, block), :] = taps
        return total + jnp.sum(taps * taps, axis=0, keepdims=True)

    total = lax.fori_loop(0, count, fill, jnp.zeros((1, n_rows), jnp.float32))
    norm = jnp.sqrt(total)
    edge_ref[:margin, :] = (raw_ref[:margin, :] / norm).astype(jnp.bfloat16)
    own_ref[...] = (raw_ref[margin : margin + n_rows, :] / norm).astype(jnp.bfloat16)
    edge_ref[margin:, :] = (raw_ref[margin + n_rows :, :] / norm).astype(jnp.bfloat16)


def span_band(band_ref):
    n_cols, in_count = band_ref.shape
    margin = 2 * SPANW
    row = lax.broadcasted_iota(jnp.int32, (n_cols, in_count), 0)
    col = lax.broadcasted_iota(jnp.int32, (n_cols, in_count), 1)
    taps = raw_taps((col - margin - row).astype(jnp.float32), float(SPANW))
    norm = jnp.sqrt(jnp.sum(taps * taps, axis=1, keepdims=True))
    band_ref[...] = (taps / norm).astype(jnp.bfloat16)


def filter_kernel(
    n_wall, n_span, noise, widths, fluct, totals,
    stage, spread, psi, halo, smooth, sides, raw, own_band, edge_band, z_band, carry, acc, sums,
    load_sem, spread_sem, meet, wall_send, wall_recv, span_send, span_recv, sum_send, sum_recv,
):
    n_comp, _, n_cols, n_rows = noise.shape
    chunks = stage.shape[0]
    half = n_rows // 2
    moments = acc.shape[0]
    w = lax.axis_index("wall")
    p = lax.axis_index("span")
    left, right = lax.rem(p + n_span - 1, n_span), lax.rem(p + 1, n_span)
    below, above = w > 0, w < n_wall - 1

    barrier = pltpu.get_barrier_semaphore()

    n_wall_first = chunks - FIRST
    plain = n_wall_first - FIRST
    early = [k for i in range(FIRST) for k in (n_wall_first + i, i)]

    def time_of(k):
        if isinstance(k, int) and k >= n_wall_first:
            return plain + 1 + 2 * (k - n_wall_first)
        return k + (k // plain) * (k - plain)

    def load(k, sem):
        return pltpu.make_async_copy(
            noise.at[:, pl.ds(time_of(k) * STEP, STEP)], stage.at[k], load_sem.at[sem]
        )

    def start_load(k, _):
        load(k, len(early)).start()
        return 0

    load_spread = pltpu.make_async_copy(widths, spread, spread_sem)
    for sem, k in enumerate(early):
        load(k, sem).start()
    load_spread.start()
    lax.fori_loop(FIRST, n_wall_first, start_load, 0)

    def signal(where, **device):
        pl.semaphore_signal(where, inc=1, device_id=device, device_id_type=MESH)

    signal(barrier, span=left)
    signal(barrier, span=right)

    @pl.when(below)
    def _():
        signal(barrier, wall=w - 1)

    @pl.when(above)
    def _():
        signal(barrier, wall=w + 1)

    rounds = (n_span // 2).bit_length() - 1

    def reach(r):
        if r < rounds:
            signal(meet.at[r], span=lax.rem(p + 2**r, n_span))
            signal(meet.at[r], span=lax.rem(p + n_span - 2**r, n_span))

    def reached(r):
        if r < rounds:
            pl.semaphore_wait(meet.at[r], 2)

    def to_above(k):
        return pltpu.make_async_remote_copy(
            src_ref=psi.at[k, 1], dst_ref=halo.at[k, 0],
            send_sem=wall_send.at[0], recv_sem=wall_recv.at[k],
            device_id={"wall": w + 1}, device_id_type=MESH,
        )

    def to_below(k):
        return pltpu.make_async_remote_copy(
            src_ref=psi.at[k, 0], dst_ref=halo.at[k, 1],
            send_sem=wall_send.at[1], recv_sem=wall_recv.at[k],
            device_id={"wall": w - 1}, device_id_type=MESH,
        )

    def to_right(k):
        return pltpu.make_async_remote_copy(
            src_ref=smooth.at[k], dst_ref=sides.at[k, 0],
            send_sem=span_send.at[0], recv_sem=span_recv.at[k],
            device_id={"span": right}, device_id_type=MESH,
        )

    def to_left(k):
        return pltpu.make_async_remote_copy(
            src_ref=smooth.at[k], dst_ref=sides.at[k, 1],
            send_sem=span_send.at[1], recv_sem=span_recv.at[k],
            device_id={"span": left}, device_id_type=MESH,
        )

    def landed(ref, sem):
        pltpu.make_async_copy(ref, ref, sem).wait()

    def convert(k, span_first):
        for c in range(n_comp):
            for s in range(STEP):
                bits = stage[k, c, s].astype(jnp.float32)
                field = (math.sqrt(12.0) * ((bits + 0.5) * INV_RANGE - 0.5)).astype(jnp.bfloat16)
                if span_first:
                    smooth[k, c * STEP + s] = field
                else:
                    at = (c * STEP + s) * n_cols
                    psi[k, 0, at : at + n_cols, :] = field[:, :half]
                    psi[k, 1, at : at + n_cols, :] = field[:, half:]

    def send_wall(k):
        @pl.when(above)
        def _():
            to_above(k).start()

        @pl.when(below)
        def _():
            to_below(k).start()

    def send_span(k):
        to_right(k).start()
        to_left(k).start()

    for sem, k in enumerate(early):
        with jax.named_scope("early_convert"):
            load(k, sem).wait()
            convert(k, k >= n_wall_first)
        if sem == 0:
            with jax.named_scope("greeted"):
                pl.semaphore_wait(barrier, 2 + below.astype(jnp.int32) + above.astype(jnp.int32))
        if k >= n_wall_first:
            send_span(k)
        else:
            send_wall(k)

    def convert_and_send(k, _):
        convert(k, False)
        send_wall(k)
        return 0

    reach(0)
    with jax.named_scope("converts"):
        landed(stage.at[pl.ds(FIRST, plain)], load_sem.at[len(early)])
        lax.fori_loop(FIRST, n_wall_first, convert_and_send, 0)
    with jax.named_scope("bands"):
        load_spread.wait()
        wall_bands(spread, raw, own_band, edge_band)
        span_band(z_band)
    carry[...] = jnp.zeros_like(carry)
    acc[...] = jnp.zeros_like(acc)

    @pl.when(jnp.logical_not(below))
    def _():
        def clear(k, _):
            halo[k, 0] = jnp.zeros(halo.shape[2:], halo.dtype)
            return 0

        lax.fori_loop(0, chunks, clear, 0)

    @pl.when(jnp.logical_not(above))
    def _():
        def clear(k, _):
            halo[k, 1] = jnp.zeros(halo.shape[2:], halo.dtype)
            return 0

        lax.fori_loop(0, chunks, clear, 0)

    def wall_arrived(k):
        @pl.when(jnp.logical_and(below, above))
        def _():
            landed(halo.at[k], wall_recv.at[k])

        @pl.when(jnp.logical_not(below))
        def _():
            landed(halo.at[k, 1], wall_recv.at[k])

        @pl.when(jnp.logical_not(above))
        def _():
            landed(halo.at[k, 0], wall_recv.at[k])

    def wall_sum(k):
        with jax.named_scope("wall_wait"):
            wall_arrived(k)
        own = jnp.concatenate([psi[k, 0], psi[k, 1]], axis=1)
        edge = jnp.concatenate([halo[k, 0], halo[k, 1]], axis=1)
        total = jnp.dot(own, own_band[...], preferred_element_type=jnp.float32) + jnp.dot(
            edge, edge_band[...], preferred_element_type=jnp.float32
        )
        return total.reshape(n_comp * STEP, n_cols, n_rows)

    def span_arrived(k):
        with jax.named_scope("span_wait"):
            landed(sides.at[k], span_recv.at[k])

    def span_sum(k, i):
        window = jnp.concatenate([sides[k, 0, i], smooth[k, i], sides[k, 1, i]], axis=0)
        return jnp.dot(z_band[...], window, preferred_element_type=jnp.float32)

    def wall_filter(k):
        smooth[k] = wall_sum(k).astype(jnp.bfloat16)
        send_span(k)

    def span_filter_first(k):
        span_arrived(k)
        for i in range(n_comp * STEP):
            field = span_sum(k, i).astype(jnp.bfloat16)
            psi[k, 0, i * n_cols : (i + 1) * n_cols, :] = field[:, :half]
            psi[k, 1, i * n_cols : (i + 1) * n_cols, :] = field[:, half:]
        send_wall(k)

    def advance(k, filtered):
        for s in range(STEP):
            t = time_of(k) * STEP + s
            fresh = jnp.where(t == 0, 1.0, FRESH)
            values = []
            for c in range(n_comp):
                value = DECAY * carry[c] + fresh * filtered(c, s)
                carry[c] = value
                fluct[c, t] = value
                values.append(value)
            for c in range(n_comp):
                acc[c] += jnp.sum(values[c].reshape(n_cols // 8, 8, n_rows), axis=0)
            for slot, (a, b) in enumerate(PAIRS):
                product = values[a] * values[b]
                acc[n_comp + slot] += jnp.sum(product.reshape(n_cols // 8, 8, n_rows), axis=0)

    def span_filter(k):
        span_arrived(k)
        advance(k, lambda c, s: span_sum(k, c * STEP + s))

    def wall_filter_last(k):
        fields = wall_sum(k)
        for c in range(n_comp):
            for s in range(STEP):
                fluct[c, time_of(k) * STEP + s] = fields[c * STEP + s]

    def middle_steps(k, _):
        wall_filter(k)
        span_filter(k - LAG)
        return 0

    def last_steps(k, _):
        span_filter(k)
        return 0

    for k in range(LAG):
        wall_filter(k)
        if k < FIRST:
            span_filter_first(n_wall_first + k)
        reached(k)
        reach(k + 1)
    lax.fori_loop(LAG, n_wall_first, middle_steps, 0)
    for r in range(LAG, rounds):
        reached(r)
        reach(r + 1)
    lax.fori_loop(n_wall_first - LAG, plain, last_steps, 0)
    for i in range(FIRST):
        wall_filter_last(n_wall_first + i)
        span_filter(plain + i)
        advance(n_wall_first + i, lambda c, s: fluct[c, time_of(n_wall_first + i) * STEP + s])

    for m in range(moments):
        sums[p, m] = jnp.sum(acc[m], axis=0, keepdims=True)

    n_y = min(4, n_span // 2)

    def rank(there):
        return there // (2 * n_y) + there // 2 % n_y

    with jax.named_scope("share"):
        for there in sorted(range(n_span), key=rank):

            @pl.when(p != there)
            def _():
                pltpu.make_async_remote_copy(
                    src_ref=sums.at[p], dst_ref=sums.at[p],
                    send_sem=sum_send, recv_sem=sum_recv,
                    device_id={"span": there}, device_id_type=MESH,
                ).start()

    with jax.named_scope("send_ends"):

        @pl.when(above)
        def _():
            landed(psi.at[:, 1], wall_send.at[0])

        @pl.when(below)
        def _():
            landed(psi.at[:, 0], wall_send.at[1])

        landed(smooth, span_send.at[0])
        landed(smooth, span_send.at[1])

    others = sums.at[pl.ds(1, n_span - 1)]
    with jax.named_scope("sums_wait"):
        landed(others, sum_recv)

    def collect(i, total):
        return total + sums[i]

    totals[...] = lax.fori_loop(1, n_span, collect, sums[0])
    with jax.named_scope("share_ends"):
        landed(others, sum_send)


def lund_transform(sample_covariance, target_factor_diagonal, target_factor_lower):
    cov_00 = sample_covariance[0] + SPREAD_FLOOR
    cov_10 = sample_covariance[1]
    cov_11 = sample_covariance[2] + SPREAD_FLOOR
    cov_20 = sample_covariance[3]
    cov_21 = sample_covariance[4]
    cov_22 = sample_covariance[5] + SPREAD_FLOOR
    chol_00 = jnp.sqrt(cov_00)
    chol_10 = cov_10 / chol_00
    chol_20 = cov_20 / chol_00
    chol_11 = jnp.sqrt(cov_11 - chol_10 * chol_10)
    chol_21 = (cov_21 - chol_20 * chol_10) / chol_11
    chol_22 = jnp.sqrt(cov_22 - chol_20 * chol_20 - chol_21 * chol_21)
    inv_00 = 1.0 / chol_00
    inv_11 = 1.0 / chol_11
    inv_22 = 1.0 / chol_22
    inv_10 = -chol_10 * inv_00 * inv_11
    inv_21 = -chol_21 * inv_11 * inv_22
    inv_20 = -(chol_20 * inv_00 + chol_21 * inv_10) * inv_22
    gain_00 = target_factor_diagonal[0] * inv_00
    gain_10 = target_factor_lower[0] * inv_00 + target_factor_diagonal[1] * inv_10
    gain_11 = target_factor_diagonal[1] * inv_11
    gain_20 = (
        target_factor_lower[1] * inv_00
        + target_factor_lower[2] * inv_10
        + target_factor_diagonal[2] * inv_20
    )
    gain_21 = target_factor_lower[2] * inv_11 + target_factor_diagonal[2] * inv_21
    gain_22 = target_factor_diagonal[2] * inv_22
    return (gain_00,), (gain_10, gain_11), (gain_20, gain_21, gain_22)


def scale_kernel(cell_count, fluct, totals, profile, diagonal, lower, out, ready, sem):
    n_comp, n_samples, n_cols, n_rows = fluct.shape
    moments = n_comp + len(PAIRS)
    row = [totals[i] / cell_count for i in range(moments)]
    means = row[:n_comp]
    spread = [row[n_comp + slot] - means[a] * means[b] for slot, (a, b) in enumerate(PAIRS)]
    factors = lund_transform(
        spread,
        [diagonal[i : i + 1, :] for i in range(3)],
        [lower[i : i + 1, :] for i in range(3)],
    )

    def one_sample(s, _):
        centred = [fluct[c, s] - means[c] for c in range(n_comp)]
        for c in range(n_comp):
            value = profile[c : c + 1, :]
            for d in range(c + 1):
                value = value + factors[c][d] * centred[d]
            ready[c, s] = value
        pltpu.make_async_copy(ready.at[:, s], out.at[:, s], sem).start()
        return 0

    lax.fori_loop(0, n_samples, one_sample, 0)
    pltpu.make_async_copy(ready, out, sem).wait()


def shards(
    noise_bits, filter_widths, target_mean_profile, target_factor_diagonal, target_factor_lower
):
    n_comp, n_samples, n_cols, n_rows = noise_bits.shape
    n_wall, n_span = lax.axis_size("wall"), lax.axis_size("span")
    chunks = n_samples // STEP
    rows = n_comp * STEP * n_cols
    half = n_rows // 2
    moments = n_comp + len(PAIRS)
    bf16, f32 = jnp.bfloat16, jnp.float32
    dma = pltpu.SemaphoreType.DMA
    fluct, totals = pl.pallas_call(
        functools.partial(filter_kernel, n_wall, n_span),
        out_shape=(
            pltpu.VMEM((n_comp, n_samples, n_cols, n_rows), f32),
            pltpu.VMEM((moments, 1, n_rows), f32),
        ),
        in_specs=[
            pl.BlockSpec(memory_space=pltpu.HBM),
            pl.BlockSpec(memory_space=pltpu.HBM),
        ],
        out_specs=(
            pl.BlockSpec(memory_space=pltpu.VMEM),
            pl.BlockSpec(memory_space=pltpu.VMEM),
        ),
        scratch_shapes=[
            pltpu.VMEM((chunks, n_comp, STEP, n_cols, n_rows), jnp.int32),
            pltpu.VMEM((1, n_rows), jnp.int32),
            pltpu.VMEM((chunks, 2, rows, half), bf16),
            pltpu.VMEM((chunks, 2, rows, half), bf16),
            pltpu.VMEM((chunks, n_comp * STEP, n_cols, n_rows), bf16),
            pltpu.VMEM((chunks, 2, n_comp * STEP, n_cols, n_rows), bf16),
            pltpu.VMEM((n_rows + 4 * WMAX, n_rows), f32),
            pltpu.VMEM((n_rows, n_rows), bf16),
            pltpu.VMEM((4 * WMAX, n_rows), bf16),
            pltpu.VMEM((n_cols, n_cols + 4 * SPANW), bf16),
            pltpu.VMEM((n_comp, n_cols, n_rows), f32),
            pltpu.VMEM((moments, 8, n_rows), f32),
            pltpu.VMEM((n_span, moments, 1, n_rows), f32),
            dma((2 * FIRST + 1,)),
            dma,
            pltpu.SemaphoreType.REGULAR((max(1, (n_span // 2).bit_length() - 1),)),
            dma((2,)),
            dma((chunks,)),
            dma((2,)),
            dma((chunks,)),
            dma,
            dma,
        ],
        compiler_params=pltpu.CompilerParams(
            collective_id=0, has_side_effects=True, vmem_limit_bytes=40 * 1024 * 1024
        ),
        name="filters",
    )(
        pltpu.with_memory_space_constraint(noise_bits, pltpu.HBM),
        pltpu.with_memory_space_constraint(filter_widths.reshape(1, n_rows), pltpu.HBM),
    )

    in_vmem = pl.BlockSpec(memory_space=pltpu.VMEM)
    return pl.pallas_call(
        functools.partial(scale_kernel, float(n_samples * n_cols * n_span)),
        out_shape=pltpu.HBM(noise_bits.shape, f32),
        in_specs=[in_vmem] * 5,
        out_specs=pl.BlockSpec(memory_space=pltpu.HBM),
        scratch_shapes=[pltpu.VMEM(noise_bits.shape, f32), dma],
        compiler_params=pltpu.CompilerParams(vmem_limit_bytes=16 * 1024 * 1024),
        name="rescale",
    )(fluct, totals, target_mean_profile, target_factor_diagonal, target_factor_lower)


def solution(mesh):
    placed = (
        P(None, None, "span", "wall"),
        P("wall"),
        P(None, "wall"),
        P(None, "wall"),
        P(None, "wall"),
    )
    return jax.shard_map(
        shards, mesh=mesh, in_specs=placed, out_specs=P(None, None, "span", "wall"), check_vma=False
    )
```

```python
import functools
import math

import jax
import jax.numpy as jnp
from jax import lax
from jax.experimental import pallas as pl
from jax.experimental.pallas import tpu as pltpu
from jax.sharding import PartitionSpec as P

WMAX = 64
SPANW = 32
TSCALE = 8
STEP = 2
LAG = 5
FIRST = 4

PAIRS = ((0, 0), (1, 0), (1, 1), (2, 0), (2, 1), (2, 2))
SPREAD_FLOOR = 0.25
INV_RANGE = 1.0 / 1073741824.0
DECAY = math.exp(-math.pi / (2.0 * TSCALE))
FRESH = math.sqrt(1.0 - DECAY * DECAY)
MESH = pl.DeviceIdType.MESH


def raw_taps(offsets, spread):
    inside = jnp.abs(offsets) <= 2.0 * spread
    safe_off = jnp.where(inside, offsets, 0.0)
    return jnp.where(
        inside, jnp.exp(-math.pi * safe_off * safe_off / (8.0 * spread * spread)), 0.0
    )


def wall_bands(widths_ref, raw_ref, own_ref, edge_ref):
    n_rows = widths_ref.shape[1]
    margin = 2 * WMAX
    block = 64
    count = (n_rows + 2 * margin) // block
    spread = widths_ref[...].astype(jnp.float32)

    def fill(i, total):
        at = pl.multiple_of(i * block, block)
        row = lax.broadcasted_iota(jnp.int32, (block, n_rows), 0) + i * block
        col = lax.broadcasted_iota(jnp.int32, (block, n_rows), 1)
        taps = raw_taps((row - margin - col).astype(jnp.float32), spread)
        raw_ref[pl.ds(at, block), :] = taps
        return total + jnp.sum(taps * taps, axis=0, keepdims=True)

    total = lax.fori_loop(0, count, fill, jnp.zeros((1, n_rows), jnp.float32))
    norm = jnp.sqrt(total)
    edge_ref[:margin, :] = (raw_ref[:margin, :] / norm).astype(jnp.bfloat16)
    own_ref[...] = (raw_ref[margin : margin + n_rows, :] / norm).astype(jnp.bfloat16)
    edge_ref[margin:, :] = (raw_ref[margin + n_rows :, :] / norm).astype(jnp.bfloat16)


def span_band(band_ref):
    n_cols, in_count = band_ref.shape
    margin = 2 * SPANW
    row = lax.broadcasted_iota(jnp.int32, (n_cols, in_count), 0)
    col = lax.broadcasted_iota(jnp.int32, (n_cols, in_count), 1)
    taps = raw_taps((col - margin - row).astype(jnp.float32), float(SPANW))
    norm = jnp.sqrt(jnp.sum(taps * taps, axis=1, keepdims=True))
    band_ref[...] = (taps / norm).astype(jnp.bfloat16)


def filter_kernel(
    n_wall, n_span, noise, widths, fluct, totals,
    stage, spread, psi, halo, smooth, sides, raw, own_band, edge_band, z_band, carry, acc, sums,
    load_sem, spread_sem, meet, wall_send, wall_recv, span_send, span_recv, sum_send, sum_recv,
):
    n_comp, _, n_cols, n_rows = noise.shape
    chunks = stage.shape[0]
    half = n_rows // 2
    moments = acc.shape[0]
    w = lax.axis_index("wall")
    p = lax.axis_index("span")
    left, right = lax.rem(p + n_span - 1, n_span), lax.rem(p + 1, n_span)
    below, above = w > 0, w < n_wall - 1

    barrier = pltpu.get_barrier_semaphore()

    def signal(where, **device):
        pl.semaphore_signal(where, inc=1, device_id=device, device_id_type=MESH)

    signal(barrier, span=left)
    signal(barrier, span=right)

    @pl.when(below)
    def _():
        signal(barrier, wall=w - 1)

    @pl.when(above)
    def _():
        signal(barrier, wall=w + 1)

    n_wall_first = chunks - FIRST
    plain = n_wall_first - FIRST
    early = [k for i in range(FIRST) for k in (n_wall_first + i, i)]

    def time_of(k):
        if isinstance(k, int) and k >= n_wall_first:
            return plain + 1 + 2 * (k - n_wall_first)
        return k + (k // plain) * (k - plain)

    def load(k, sem):
        return pltpu.make_async_copy(
            noise.at[:, pl.ds(time_of(k) * STEP, STEP)], stage.at[k], load_sem.at[sem]
        )

    def start_load(k, _):
        load(k, len(early)).start()
        return 0

    load_spread = pltpu.make_async_copy(widths, spread, spread_sem)
    for sem, k in enumerate(early):
        load(k, sem).start()
    load_spread.start()
    lax.fori_loop(FIRST, n_wall_first, start_load, 0)

    rounds = (n_span // 2).bit_length() - 1

    def reach(r):
        if r < rounds:
            signal(meet.at[r], span=lax.rem(p + 2**r, n_span))
            signal(meet.at[r], span=lax.rem(p + n_span - 2**r, n_span))

    def reached(r):
        if r < rounds:
            pl.semaphore_wait(meet.at[r], 2)

    def to_above(k):
        return pltpu.make_async_remote_copy(
            src_ref=psi.at[k, 1], dst_ref=halo.at[k, 0],
            send_sem=wall_send.at[0], recv_sem=wall_recv.at[k],
            device_id={"wall": w + 1}, device_id_type=MESH,
        )

    def to_below(k):
        return pltpu.make_async_remote_copy(
            src_ref=psi.at[k, 0], dst_ref=halo.at[k, 1],
            send_sem=wall_send.at[1], recv_sem=wall_recv.at[k],
            device_id={"wall": w - 1}, device_id_type=MESH,
        )

    def to_right(k):
        return pltpu.make_async_remote_copy(
            src_ref=smooth.at[k], dst_ref=sides.at[k, 0],
            send_sem=span_send.at[0], recv_sem=span_recv.at[k],
            device_id={"span": right}, device_id_type=MESH,
        )

    def to_left(k):
        return pltpu.make_async_remote_copy(
            src_ref=smooth.at[k], dst_ref=sides.at[k, 1],
            send_sem=span_send.at[1], recv_sem=span_recv.at[k],
            device_id={"span": left}, device_id_type=MESH,
        )

    def landed(ref, sem):
        pltpu.make_async_copy(ref, ref, sem).wait()

    def convert(k, span_first):
        for c in range(n_comp):
            for s in range(STEP):
                bits = stage[k, c, s].astype(jnp.float32)
                field = (math.sqrt(12.0) * ((bits + 0.5) * INV_RANGE - 0.5)).astype(jnp.bfloat16)
                if span_first:
                    smooth[k, c * STEP + s] = field
                else:
                    at = (c * STEP + s) * n_cols
                    psi[k, 0, at : at + n_cols, :] = field[:, :half]
                    psi[k, 1, at : at + n_cols, :] = field[:, half:]

    def send_wall(k):
        @pl.when(above)
        def _():
            to_above(k).start()

        @pl.when(below)
        def _():
            to_below(k).start()

    def send_span(k):
        to_right(k).start()
        to_left(k).start()

    for sem, k in enumerate(early):
        with jax.named_scope("early_convert"):
            load(k, sem).wait()
            convert(k, k >= n_wall_first)
        if sem == 0:
            with jax.named_scope("greeted"):
                pl.semaphore_wait(barrier, 2 + below.astype(jnp.int32) + above.astype(jnp.int32))
        if k >= n_wall_first:
            send_span(k)
        else:
            send_wall(k)

    def convert_and_send(k, _):
        convert(k, False)
        send_wall(k)
        return 0

    reach(0)
    with jax.named_scope("converts"):
        landed(stage.at[pl.ds(FIRST, plain)], load_sem.at[len(early)])
        lax.fori_loop(FIRST, n_wall_first, convert_and_send, 0)
    with jax.named_scope("bands"):
        load_spread.wait()
        wall_bands(spread, raw, own_band, edge_band)
        span_band(z_band)
    carry[...] = jnp.zeros_like(carry)
    acc[...] = jnp.zeros_like(acc)

    @pl.when(jnp.logical_not(below))
    def _():
        def clear(k, _):
            halo[k, 0] = jnp.zeros(halo.shape[2:], halo.dtype)
            return 0

        lax.fori_loop(0, chunks, clear, 0)

    @pl.when(jnp.logical_not(above))
    def _():
        def clear(k, _):
            halo[k, 1] = jnp.zeros(halo.shape[2:], halo.dtype)
            return 0

        lax.fori_loop(0, chunks, clear, 0)

    def wall_arrived(k):
        @pl.when(jnp.logical_and(below, above))
        def _():
            landed(halo.at[k], wall_recv.at[k])

        @pl.when(jnp.logical_not(below))
        def _():
            landed(halo.at[k, 1], wall_recv.at[k])

        @pl.when(jnp.logical_not(above))
        def _():
            landed(halo.at[k, 0], wall_recv.at[k])

    def wall_sum(k):
        with jax.named_scope("wall_wait"):
            wall_arrived(k)
        own = jnp.concatenate([psi[k, 0], psi[k, 1]], axis=1)
        edge = jnp.concatenate([halo[k, 0], halo[k, 1]], axis=1)
        total = jnp.dot(own, own_band[...], preferred_element_type=jnp.float32) + jnp.dot(
            edge, edge_band[...], preferred_element_type=jnp.float32
        )
        return total.reshape(n_comp * STEP, n_cols, n_rows)

    def span_arrived(k):
        with jax.named_scope("span_wait"):
            landed(sides.at[k], span_recv.at[k])

    def span_sum(k, i):
        window = jnp.concatenate([sides[k, 0, i], smooth[k, i], sides[k, 1, i]], axis=0)
        return jnp.dot(z_band[...], window, preferred_element_type=jnp.float32)

    def wall_filter(k):
        smooth[k] = wall_sum(k).astype(jnp.bfloat16)
        send_span(k)

    def span_filter_first(k):
        span_arrived(k)
        for i in range(n_comp * STEP):
            field = span_sum(k, i).astype(jnp.bfloat16)
            psi[k, 0, i * n_cols : (i + 1) * n_cols, :] = field[:, :half]
            psi[k, 1, i * n_cols : (i + 1) * n_cols, :] = field[:, half:]
        send_wall(k)

    def advance(k, filtered):
        for s in range(STEP):
            t = time_of(k) * STEP + s
            fresh = jnp.where(t == 0, 1.0, FRESH)
            values = []
            for c in range(n_comp):
                value = DECAY * carry[c] + fresh * filtered(c, s)
                carry[c] = value
                fluct[c, t] = value
                values.append(value)
            for c in range(n_comp):
                acc[c] += jnp.sum(values[c].reshape(n_cols // 8, 8, n_rows), axis=0)
            for slot, (a, b) in enumerate(PAIRS):
                product = values[a] * values[b]
                acc[n_comp + slot] += jnp.sum(product.reshape(n_cols // 8, 8, n_rows), axis=0)

    def span_filter(k):
        span_arrived(k)
        advance(k, lambda c, s: span_sum(k, c * STEP + s))

    def wall_filter_last(k):
        fields = wall_sum(k)
        for c in range(n_comp):
            for s in range(STEP):
                fluct[c, time_of(k) * STEP + s] = fields[c * STEP + s]

    def middle_steps(k, _):
        wall_filter(k)
        span_filter(k - LAG)
        return 0

    def last_steps(k, _):
        span_filter(k)
        return 0

    for k in range(LAG):
        wall_filter(k)
        if k < FIRST:
            span_filter_first(n_wall_first + k)
        reached(k)
        reach(k + 1)
    lax.fori_loop(LAG, n_wall_first, middle_steps, 0)
    for r in range(LAG, rounds):
        reached(r)
        reach(r + 1)
    lax.fori_loop(n_wall_first - LAG, plain, last_steps, 0)
    for i in range(FIRST):
        wall_filter_last(n_wall_first + i)
        span_filter(plain + i)
        advance(n_wall_first + i, lambda c, s: fluct[c, time_of(n_wall_first + i) * STEP + s])

    for m in range(moments):
        sums[p, m] = jnp.sum(acc[m], axis=0, keepdims=True)

    n_y = min(4, n_span // 2)

    n_x = n_span // (2 * n_y)
    in_group = 2 * n_y
    group = p // in_group

    def rank(there):
        return there // in_group + there // 2 % n_y

    with jax.named_scope("share"):
        for there in sorted(range(n_span), key=rank):

            @pl.when(p != there)
            def _():
                pltpu.make_async_remote_copy(
                    src_ref=sums.at[p], dst_ref=sums.at[p],
                    send_sem=sum_send, recv_sem=sum_recv.at[group],
                    device_id={"span": there}, device_id_type=MESH,
                ).start()

    with jax.named_scope("send_ends"):

        @pl.when(above)
        def _():
            landed(psi.at[:, 1], wall_send.at[0])

        @pl.when(below)
        def _():
            landed(psi.at[:, 0], wall_send.at[1])

        landed(smooth, span_send.at[0])
        landed(smooth, span_send.at[1])

    def collect(i, total):
        return total + sums[i]

    total = jnp.zeros(sums.shape[1:], jnp.float32)
    with jax.named_scope("sums_wait"):
        for g in range(n_x):

            @pl.when(group == g)
            def _():
                landed(sums.at[pl.ds(0, in_group - 1)], sum_recv.at[g])

            @pl.when(group != g)
            def _():
                landed(sums.at[pl.ds(0, in_group)], sum_recv.at[g])

            total = lax.fori_loop(g * in_group, (g + 1) * in_group, collect, total)
    totals[...] = total
    with jax.named_scope("share_ends"):
        landed(sums.at[pl.ds(0, n_span - 1)], sum_send)


def lund_transform(sample_covariance, target_factor_diagonal, target_factor_lower):
    cov_00 = sample_covariance[0] + SPREAD_FLOOR
    cov_10 = sample_covariance[1]
    cov_11 = sample_covariance[2] + SPREAD_FLOOR
    cov_20 = sample_covariance[3]
    cov_21 = sample_covariance[4]
    cov_22 = sample_covariance[5] + SPREAD_FLOOR
    inv_00 = lax.rsqrt(cov_00)
    chol_10 = cov_10 * inv_00
    chol_20 = cov_20 * inv_00
    inv_11 = lax.rsqrt(cov_11 - chol_10 * chol_10)
    chol_21 = (cov_21 - chol_20 * chol_10) * inv_11
    inv_22 = lax.rsqrt(cov_22 - chol_20 * chol_20 - chol_21 * chol_21)
    inv_10 = -chol_10 * inv_00 * inv_11
    inv_21 = -chol_21 * inv_11 * inv_22
    inv_20 = -(chol_20 * inv_00 + chol_21 * inv_10) * inv_22
    gain_00 = target_factor_diagonal[0] * inv_00
    gain_10 = target_factor_lower[0] * inv_00 + target_factor_diagonal[1] * inv_10
    gain_11 = target_factor_diagonal[1] * inv_11
    gain_20 = (
        target_factor_lower[1] * inv_00
        + target_factor_lower[2] * inv_10
        + target_factor_diagonal[2] * inv_20
    )
    gain_21 = target_factor_lower[2] * inv_11 + target_factor_diagonal[2] * inv_21
    gain_22 = target_factor_diagonal[2] * inv_22
    return (gain_00,), (gain_10, gain_11), (gain_20, gain_21, gain_22)


def scale_kernel(cell_count, fluct, totals, profile, diagonal, lower, out, ready, sem):
    n_comp, n_samples, n_cols, n_rows = fluct.shape
    moments = n_comp + len(PAIRS)
    row = [totals[i] * (1.0 / cell_count) for i in range(moments)]
    means = row[:n_comp]
    spread = [row[n_comp + slot] - means[a] * means[b] for slot, (a, b) in enumerate(PAIRS)]
    factors = lund_transform(
        spread,
        [diagonal[i : i + 1, :] for i in range(3)],
        [lower[i : i + 1, :] for i in range(3)],
    )

    def one_sample(s, _):
        centred = [fluct[c, s] - means[c] for c in range(n_comp)]
        for c in range(n_comp):
            value = profile[c : c + 1, :]
            for d in range(c + 1):
                value = value + factors[c][d] * centred[d]
            ready[c, s] = value
        pltpu.make_async_copy(ready.at[:, s], out.at[:, s], sem).start()
        return 0

    lax.fori_loop(0, n_samples, one_sample, 0)
    pltpu.make_async_copy(ready, out, sem).wait()


def shards(
    noise_bits, filter_widths, target_mean_profile, target_factor_diagonal, target_factor_lower
):
    n_comp, n_samples, n_cols, n_rows = noise_bits.shape
    n_wall, n_span = lax.axis_size("wall"), lax.axis_size("span")
    chunks = n_samples // STEP
    rows = n_comp * STEP * n_cols
    half = n_rows // 2
    moments = n_comp + len(PAIRS)
    bf16, f32 = jnp.bfloat16, jnp.float32
    dma = pltpu.SemaphoreType.DMA
    fluct, totals = pl.pallas_call(
        functools.partial(filter_kernel, n_wall, n_span),
        out_shape=(
            pltpu.VMEM((n_comp, n_samples, n_cols, n_rows), f32),
            pltpu.VMEM((moments, 1, n_rows), f32),
        ),
        in_specs=[
            pl.BlockSpec(memory_space=pltpu.HBM),
            pl.BlockSpec(memory_space=pltpu.HBM),
        ],
        out_specs=(
            pl.BlockSpec(memory_space=pltpu.VMEM),
            pl.BlockSpec(memory_space=pltpu.VMEM),
        ),
        scratch_shapes=[
            pltpu.VMEM((chunks, n_comp, STEP, n_cols, n_rows), jnp.int32),
            pltpu.VMEM((1, n_rows), jnp.int32),
            pltpu.VMEM((chunks, 2, rows, half), bf16),
            pltpu.VMEM((chunks, 2, rows, half), bf16),
            pltpu.VMEM((chunks, n_comp * STEP, n_cols, n_rows), bf16),
            pltpu.VMEM((chunks, 2, n_comp * STEP, n_cols, n_rows), bf16),
            pltpu.VMEM((n_rows + 4 * WMAX, n_rows), f32),
            pltpu.VMEM((n_rows, n_rows), bf16),
            pltpu.VMEM((4 * WMAX, n_rows), bf16),
            pltpu.VMEM((n_cols, n_cols + 4 * SPANW), bf16),
            pltpu.VMEM((n_comp, n_cols, n_rows), f32),
            pltpu.VMEM((moments, 8, n_rows), f32),
            pltpu.VMEM((n_span, moments, 1, n_rows), f32),
            dma((2 * FIRST + 1,)),
            dma,
            pltpu.SemaphoreType.REGULAR((max(1, (n_span // 2).bit_length() - 1),)),
            dma((2,)),
            dma((chunks,)),
            dma((2,)),
            dma((chunks,)),
            dma,
            dma((4,)),
        ],
        compiler_params=pltpu.CompilerParams(
            collective_id=0, has_side_effects=True, vmem_limit_bytes=40 * 1024 * 1024
        ),
        name="filters",
    )(
        pltpu.with_memory_space_constraint(noise_bits, pltpu.HBM),
        pltpu.with_memory_space_constraint(filter_widths.reshape(1, n_rows), pltpu.HBM),
    )

    in_vmem = pl.BlockSpec(memory_space=pltpu.VMEM)
    return pl.pallas_call(
        functools.partial(scale_kernel, float(n_samples * n_cols * n_span)),
        out_shape=pltpu.HBM(noise_bits.shape, f32),
        in_specs=[in_vmem] * 5,
        out_specs=pl.BlockSpec(memory_space=pltpu.HBM),
        scratch_shapes=[pltpu.VMEM(noise_bits.shape, f32), dma],
        compiler_params=pltpu.CompilerParams(vmem_limit_bytes=16 * 1024 * 1024),
        name="rescale",
    )(fluct, totals, target_mean_profile, target_factor_diagonal, target_factor_lower)


def solution(mesh):
    placed = (
        P(None, None, "span", "wall"),
        P("wall"),
        P(None, "wall"),
        P(None, "wall"),
        P(None, "wall"),
    )
    return jax.shard_map(
        shards, mesh=mesh, in_specs=placed, out_specs=P(None, None, "span", "wall"), check_vma=False
    )
```

```python
import functools
import math

import jax
import jax.numpy as jnp
from jax import lax
from jax.experimental import pallas as pl
from jax.experimental.pallas import tpu as pltpu
from jax.sharding import PartitionSpec as P

WMAX = 64
SPANW = 32
TSCALE = 8
STEP = 2
LAG = 5
FIRST = 4

PAIRS = ((0, 0), (1, 0), (1, 1), (2, 0), (2, 1), (2, 2))
SPREAD_FLOOR = 0.25
INV_RANGE = 1.0 / 1073741824.0
DECAY = math.exp(-math.pi / (2.0 * TSCALE))
FRESH = math.sqrt(1.0 - DECAY * DECAY)
MESH = pl.DeviceIdType.MESH


def raw_taps(offsets, spread):
    inside = jnp.abs(offsets) <= 2.0 * spread
    safe_off = jnp.where(inside, offsets, 0.0)
    return jnp.where(
        inside, jnp.exp(-math.pi * safe_off * safe_off / (8.0 * spread * spread)), 0.0
    )


def wall_bands(widths_ref, raw_ref, own_ref, edge_ref):
    n_rows = widths_ref.shape[1]
    margin = 2 * WMAX
    block = 64
    count = (n_rows + 2 * margin) // block
    spread = widths_ref[...].astype(jnp.float32)

    def fill(i, total):
        at = pl.multiple_of(i * block, block)
        row = lax.broadcasted_iota(jnp.int32, (block, n_rows), 0) + i * block
        col = lax.broadcasted_iota(jnp.int32, (block, n_rows), 1)
        taps = raw_taps((row - margin - col).astype(jnp.float32), spread)
        raw_ref[pl.ds(at, block), :] = taps
        return total + jnp.sum(taps * taps, axis=0, keepdims=True)

    total = lax.fori_loop(0, count, fill, jnp.zeros((1, n_rows), jnp.float32))
    norm = jnp.sqrt(total)
    edge_ref[:margin, :] = (raw_ref[:margin, :] / norm).astype(jnp.bfloat16)
    own_ref[...] = (raw_ref[margin : margin + n_rows, :] / norm).astype(jnp.bfloat16)
    edge_ref[margin:, :] = (raw_ref[margin + n_rows :, :] / norm).astype(jnp.bfloat16)


def span_band(band_ref):
    n_cols, in_count = band_ref.shape
    margin = 2 * SPANW
    row = lax.broadcasted_iota(jnp.int32, (n_cols, in_count), 0)
    col = lax.broadcasted_iota(jnp.int32, (n_cols, in_count), 1)
    taps = raw_taps((col - margin - row).astype(jnp.float32), float(SPANW))
    norm = jnp.sqrt(jnp.sum(taps * taps, axis=1, keepdims=True))
    band_ref[...] = (taps / norm).astype(jnp.bfloat16)


def filter_kernel(
    n_wall, n_span, noise, widths, fluct, totals,
    stage, spread, psi, halo, smooth, sides, raw, own_band, edge_band, z_band, acc, sums,
    load_sem, spread_sem, meet, wall_send, wall_recv, span_send, span_recv, sum_send, sum_recv,
):
    n_comp, n_samples, n_cols, n_rows = noise.shape
    chunks = stage.shape[0]
    half = n_rows // 2
    moments = acc.shape[0]
    w = lax.axis_index("wall")
    p = lax.axis_index("span")
    left, right = lax.rem(p + n_span - 1, n_span), lax.rem(p + 1, n_span)
    below, above = w > 0, w < n_wall - 1

    barrier = pltpu.get_barrier_semaphore()

    def signal(where, **device):
        pl.semaphore_signal(where, inc=1, device_id=device, device_id_type=MESH)

    signal(barrier, span=left)
    signal(barrier, span=right)

    @pl.when(below)
    def _():
        signal(barrier, wall=w - 1)

    @pl.when(above)
    def _():
        signal(barrier, wall=w + 1)

    n_wall_first = chunks - FIRST
    plain = n_wall_first - FIRST
    early = [k for i in range(FIRST) for k in (n_wall_first + i, i)]

    def time_of(k):
        if isinstance(k, int) and k >= n_wall_first:
            return plain + 1 + 2 * (k - n_wall_first)
        return k + (k // plain) * (k - plain)

    def load(k, sem):
        return pltpu.make_async_copy(
            noise.at[:, pl.ds(time_of(k) * STEP, STEP)], stage.at[k], load_sem.at[sem]
        )

    def start_load(k, _):
        load(k, len(early)).start()
        return 0

    load_spread = pltpu.make_async_copy(widths, spread, spread_sem)
    for sem, k in enumerate(early):
        load(k, sem).start()
    load_spread.start()
    lax.fori_loop(FIRST, n_wall_first, start_load, 0)

    rounds = (n_span // 2).bit_length() - 1

    def reach(r):
        if r < rounds:
            signal(meet.at[r], span=lax.rem(p + 2**r, n_span))
            signal(meet.at[r], span=lax.rem(p + n_span - 2**r, n_span))

    def reached(r):
        if r < rounds:
            pl.semaphore_wait(meet.at[r], 2)

    def to_above(k):
        return pltpu.make_async_remote_copy(
            src_ref=psi.at[k, 1], dst_ref=halo.at[k, 0],
            send_sem=wall_send.at[0], recv_sem=wall_recv.at[k],
            device_id={"wall": w + 1}, device_id_type=MESH,
        )

    def to_below(k):
        return pltpu.make_async_remote_copy(
            src_ref=psi.at[k, 0], dst_ref=halo.at[k, 1],
            send_sem=wall_send.at[1], recv_sem=wall_recv.at[k],
            device_id={"wall": w - 1}, device_id_type=MESH,
        )

    def to_right(k):
        return pltpu.make_async_remote_copy(
            src_ref=smooth.at[k], dst_ref=sides.at[k, 0],
            send_sem=span_send.at[0], recv_sem=span_recv.at[k],
            device_id={"span": right}, device_id_type=MESH,
        )

    def to_left(k):
        return pltpu.make_async_remote_copy(
            src_ref=smooth.at[k], dst_ref=sides.at[k, 1],
            send_sem=span_send.at[1], recv_sem=span_recv.at[k],
            device_id={"span": left}, device_id_type=MESH,
        )

    def landed(ref, sem):
        pltpu.make_async_copy(ref, ref, sem).wait()

    def convert(k, span_first):
        for c in range(n_comp):
            for s in range(STEP):
                bits = stage[k, c, s].astype(jnp.float32)
                field = (math.sqrt(12.0) * ((bits + 0.5) * INV_RANGE - 0.5)).astype(jnp.bfloat16)
                if span_first:
                    smooth[k, c * STEP + s] = field
                else:
                    at = (c * STEP + s) * n_cols
                    psi[k, 0, at : at + n_cols, :] = field[:, :half]
                    psi[k, 1, at : at + n_cols, :] = field[:, half:]

    def send_wall(k):
        @pl.when(above)
        def _():
            to_above(k).start()

        @pl.when(below)
        def _():
            to_below(k).start()

    def send_span(k):
        to_right(k).start()
        to_left(k).start()

    for sem, k in enumerate(early):
        with jax.named_scope("early_convert"):
            load(k, sem).wait()
            convert(k, k >= n_wall_first)
        if sem == 0:
            with jax.named_scope("greeted"):
                pl.semaphore_wait(barrier, 2 + below.astype(jnp.int32) + above.astype(jnp.int32))
        if k >= n_wall_first:
            send_span(k)
        else:
            send_wall(k)

    def convert_and_send(k, _):
        convert(k, False)
        send_wall(k)
        return 0

    reach(0)
    with jax.named_scope("converts"):
        landed(stage.at[pl.ds(FIRST, plain)], load_sem.at[len(early)])
        lax.fori_loop(FIRST, n_wall_first, convert_and_send, 0)
    with jax.named_scope("bands"):
        load_spread.wait()
        wall_bands(spread, raw, own_band, edge_band)
        span_band(z_band)
    acc[...] = jnp.zeros_like(acc)

    @pl.when(jnp.logical_not(below))
    def _():
        def clear(k, _):
            halo[k, 0] = jnp.zeros(halo.shape[2:], halo.dtype)
            return 0

        lax.fori_loop(0, chunks, clear, 0)

    @pl.when(jnp.logical_not(above))
    def _():
        def clear(k, _):
            halo[k, 1] = jnp.zeros(halo.shape[2:], halo.dtype)
            return 0

        lax.fori_loop(0, chunks, clear, 0)

    def wall_arrived(k):
        @pl.when(jnp.logical_and(below, above))
        def _():
            landed(halo.at[k], wall_recv.at[k])

        @pl.when(jnp.logical_not(below))
        def _():
            landed(halo.at[k, 1], wall_recv.at[k])

        @pl.when(jnp.logical_not(above))
        def _():
            landed(halo.at[k, 0], wall_recv.at[k])

    def wall_sum(k):
        with jax.named_scope("wall_wait"):
            wall_arrived(k)
        own = jnp.concatenate([psi[k, 0], psi[k, 1]], axis=1)
        edge = jnp.concatenate([halo[k, 0], halo[k, 1]], axis=1)
        total = jnp.dot(own, own_band[...], preferred_element_type=jnp.float32) + jnp.dot(
            edge, edge_band[...], preferred_element_type=jnp.float32
        )
        return total.reshape(n_comp * STEP, n_cols, n_rows)

    def span_arrived(k):
        with jax.named_scope("span_wait"):
            landed(sides.at[k], span_recv.at[k])

    def span_sum(k, i):
        window = jnp.concatenate([sides[k, 0, i], smooth[k, i], sides[k, 1, i]], axis=0)
        return jnp.dot(z_band[...], window, preferred_element_type=jnp.float32)

    def wall_filter(k):
        smooth[k] = wall_sum(k).astype(jnp.bfloat16)
        send_span(k)

    def span_filter_first(k):
        span_arrived(k)
        for i in range(n_comp * STEP):
            field = span_sum(k, i).astype(jnp.bfloat16)
            psi[k, 0, i * n_cols : (i + 1) * n_cols, :] = field[:, :half]
            psi[k, 1, i * n_cols : (i + 1) * n_cols, :] = field[:, half:]
        send_wall(k)

    def advance(k, filtered):
        for s in range(STEP):
            t = time_of(k) * STEP + s
            fresh = jnp.where(t == 0, 1.0, FRESH)
            values = []
            for c in range(n_comp):
                earlier = fluct[c, lax.rem(t + n_samples - 1, n_samples)]
                kept = jnp.where(t == 0, 0.0, DECAY * earlier)
                value = kept + fresh * filtered(c, s)
                fluct[c, t] = value
                values.append(value)
            for c in range(n_comp):
                acc[c] += jnp.sum(values[c].reshape(n_cols // 8, 8, n_rows), axis=0)
            for slot, (a, b) in enumerate(PAIRS):
                product = values[a] * values[b]
                acc[n_comp + slot] += jnp.sum(product.reshape(n_cols // 8, 8, n_rows), axis=0)

    def span_filter(k):
        span_arrived(k)
        advance(k, lambda c, s: span_sum(k, c * STEP + s))

    def wall_filter_last(k):
        fields = wall_sum(k)
        for c in range(n_comp):
            for s in range(STEP):
                fluct[c, time_of(k) * STEP + s] = fields[c * STEP + s]

    def middle_steps(k, _):
        wall_filter(k)
        span_filter(k - LAG)
        return 0

    def last_steps(k, _):
        span_filter(k)
        return 0

    for k in range(LAG):
        wall_filter(k)
        if k < FIRST:
            span_filter_first(n_wall_first + k)
        reached(k)
        reach(k + 1)
    lax.fori_loop(LAG, n_wall_first, middle_steps, 0)
    for r in range(LAG, rounds):
        reached(r)
        reach(r + 1)
    lax.fori_loop(n_wall_first - LAG, plain, last_steps, 0)
    for i in range(FIRST):
        wall_filter_last(n_wall_first + i)
        span_filter(plain + i)
        advance(n_wall_first + i, lambda c, s: fluct[c, time_of(n_wall_first + i) * STEP + s])

    for m in range(moments):
        sums[p, m] = jnp.sum(acc[m], axis=0, keepdims=True)

    n_y = min(4, n_span // 2)

    n_x = n_span // (2 * n_y)
    in_group = 2 * n_y
    group = p // in_group

    def rank(there):
        return there // in_group + there // 2 % n_y

    with jax.named_scope("share"):
        for there in sorted(range(n_span), key=rank):

            @pl.when(p != there)
            def _():
                pltpu.make_async_remote_copy(
                    src_ref=sums.at[p], dst_ref=sums.at[p],
                    send_sem=sum_send, recv_sem=sum_recv.at[group],
                    device_id={"span": there}, device_id_type=MESH,
                ).start()

    with jax.named_scope("send_ends"):

        @pl.when(above)
        def _():
            landed(psi.at[:, 1], wall_send.at[0])

        @pl.when(below)
        def _():
            landed(psi.at[:, 0], wall_send.at[1])

        landed(smooth, span_send.at[0])
        landed(smooth, span_send.at[1])

    def collect(i, total):
        return total + sums[i]

    total = jnp.zeros(sums.shape[1:], jnp.float32)
    with jax.named_scope("sums_wait"):
        for g in range(n_x):

            @pl.when(group == g)
            def _():
                landed(sums.at[pl.ds(0, in_group - 1)], sum_recv.at[g])

            @pl.when(group != g)
            def _():
                landed(sums.at[pl.ds(0, in_group)], sum_recv.at[g])

            total = lax.fori_loop(g * in_group, (g + 1) * in_group, collect, total)
    totals[...] = total
    with jax.named_scope("share_ends"):
        landed(sums.at[pl.ds(0, n_span - 1)], sum_send)


def lund_transform(sample_covariance, target_factor_diagonal, target_factor_lower):
    cov_00 = sample_covariance[0] + SPREAD_FLOOR
    cov_10 = sample_covariance[1]
    cov_11 = sample_covariance[2] + SPREAD_FLOOR
    cov_20 = sample_covariance[3]
    cov_21 = sample_covariance[4]
    cov_22 = sample_covariance[5] + SPREAD_FLOOR
    inv_00 = lax.rsqrt(cov_00)
    chol_10 = cov_10 * inv_00
    chol_20 = cov_20 * inv_00
    inv_11 = lax.rsqrt(cov_11 - chol_10 * chol_10)
    chol_21 = (cov_21 - chol_20 * chol_10) * inv_11
    inv_22 = lax.rsqrt(cov_22 - chol_20 * chol_20 - chol_21 * chol_21)
    inv_10 = -chol_10 * inv_00 * inv_11
    inv_21 = -chol_21 * inv_11 * inv_22
    inv_20 = -(chol_20 * inv_00 + chol_21 * inv_10) * inv_22
    gain_00 = target_factor_diagonal[0] * inv_00
    gain_10 = target_factor_lower[0] * inv_00 + target_factor_diagonal[1] * inv_10
    gain_11 = target_factor_diagonal[1] * inv_11
    gain_20 = (
        target_factor_lower[1] * inv_00
        + target_factor_lower[2] * inv_10
        + target_factor_diagonal[2] * inv_20
    )
    gain_21 = target_factor_lower[2] * inv_11 + target_factor_diagonal[2] * inv_21
    gain_22 = target_factor_diagonal[2] * inv_22
    return (gain_00,), (gain_10, gain_11), (gain_20, gain_21, gain_22)


def scale_kernel(cell_count, fluct, totals, profile, diagonal, lower, out, ready, sem):
    n_comp, n_samples, n_cols, n_rows = fluct.shape
    moments = n_comp + len(PAIRS)
    row = [totals[i] * (1.0 / cell_count) for i in range(moments)]
    means = row[:n_comp]
    spread = [row[n_comp + slot] - means[a] * means[b] for slot, (a, b) in enumerate(PAIRS)]
    factors = lund_transform(
        spread,
        [diagonal[i : i + 1, :] for i in range(3)],
        [lower[i : i + 1, :] for i in range(3)],
    )

    def one_sample(s, _):
        centred = [fluct[c, s] - means[c] for c in range(n_comp)]
        for c in range(n_comp):
            value = profile[c : c + 1, :]
            for d in range(c + 1):
                value = value + factors[c][d] * centred[d]
            ready[c, s] = value
        pltpu.make_async_copy(ready.at[:, s], out.at[:, s], sem).start()
        return 0

    lax.fori_loop(0, n_samples, one_sample, 0)
    pltpu.make_async_copy(ready, out, sem).wait()


def shards(
    noise_bits, filter_widths, target_mean_profile, target_factor_diagonal, target_factor_lower
):
    n_comp, n_samples, n_cols, n_rows = noise_bits.shape
    n_wall, n_span = lax.axis_size("wall"), lax.axis_size("span")
    chunks = n_samples // STEP
    rows = n_comp * STEP * n_cols
    half = n_rows // 2
    moments = n_comp + len(PAIRS)
    bf16, f32 = jnp.bfloat16, jnp.float32
    dma = pltpu.SemaphoreType.DMA
    fluct, totals = pl.pallas_call(
        functools.partial(filter_kernel, n_wall, n_span),
        out_shape=(
            pltpu.VMEM((n_comp, n_samples, n_cols, n_rows), f32),
            pltpu.VMEM((moments, 1, n_rows), f32),
        ),
        in_specs=[
            pl.BlockSpec(memory_space=pltpu.HBM),
            pl.BlockSpec(memory_space=pltpu.HBM),
        ],
        out_specs=(
            pl.BlockSpec(memory_space=pltpu.VMEM),
            pl.BlockSpec(memory_space=pltpu.VMEM),
        ),
        scratch_shapes=[
            pltpu.VMEM((chunks, n_comp, STEP, n_cols, n_rows), jnp.int32),
            pltpu.VMEM((1, n_rows), jnp.int32),
            pltpu.VMEM((chunks, 2, rows, half), bf16),
            pltpu.VMEM((chunks, 2, rows, half), bf16),
            pltpu.VMEM((chunks, n_comp * STEP, n_cols, n_rows), bf16),
            pltpu.VMEM((chunks, 2, n_comp * STEP, n_cols, n_rows), bf16),
            pltpu.VMEM((n_rows + 4 * WMAX, n_rows), f32),
            pltpu.VMEM((n_rows, n_rows), bf16),
            pltpu.VMEM((4 * WMAX, n_rows), bf16),
            pltpu.VMEM((n_cols, n_cols + 4 * SPANW), bf16),
            pltpu.VMEM((moments, 8, n_rows), f32),
            pltpu.VMEM((n_span, moments, 1, n_rows), f32),
            dma((2 * FIRST + 1,)),
            dma,
            pltpu.SemaphoreType.REGULAR((max(1, (n_span // 2).bit_length() - 1),)),
            dma((2,)),
            dma((chunks,)),
            dma((2,)),
            dma((chunks,)),
            dma,
            dma((4,)),
        ],
        compiler_params=pltpu.CompilerParams(
            collective_id=0, has_side_effects=True, vmem_limit_bytes=40 * 1024 * 1024
        ),
        name="filters",
    )(
        pltpu.with_memory_space_constraint(noise_bits, pltpu.HBM),
        pltpu.with_memory_space_constraint(filter_widths.reshape(1, n_rows), pltpu.HBM),
    )

    in_vmem = pl.BlockSpec(memory_space=pltpu.VMEM)
    return pl.pallas_call(
        functools.partial(scale_kernel, float(n_samples * n_cols * n_span)),
        out_shape=pltpu.HBM(noise_bits.shape, f32),
        in_specs=[in_vmem] * 5,
        out_specs=pl.BlockSpec(memory_space=pltpu.HBM),
        scratch_shapes=[pltpu.VMEM(noise_bits.shape, f32), dma],
        compiler_params=pltpu.CompilerParams(vmem_limit_bytes=16 * 1024 * 1024),
        name="rescale",
    )(fluct, totals, target_mean_profile, target_factor_diagonal, target_factor_lower)


def solution(mesh):
    placed = (
        P(None, None, "span", "wall"),
        P("wall"),
        P(None, "wall"),
        P(None, "wall"),
        P(None, "wall"),
    )
    return jax.shard_map(
        shards, mesh=mesh, in_specs=placed, out_specs=P(None, None, "span", "wall"), check_vma=False
    )
```

```python
import functools
import math

import jax
import jax.numpy as jnp
from jax import lax
from jax.experimental import pallas as pl
from jax.experimental.pallas import tpu as pltpu
from jax.sharding import PartitionSpec as P

WMAX = 64
SPANW = 32
TSCALE = 8
STEP = 2
LAG = 5
FIRST = 5

PAIRS = ((0, 0), (1, 0), (1, 1), (2, 0), (2, 1), (2, 2))
SPREAD_FLOOR = 0.25
INV_RANGE = 1.0 / 1073741824.0
DECAY = math.exp(-math.pi / (2.0 * TSCALE))
FRESH = math.sqrt(1.0 - DECAY * DECAY)
MESH = pl.DeviceIdType.MESH


def raw_taps(offsets, spread):
    inside = jnp.abs(offsets) <= 2.0 * spread
    safe_off = jnp.where(inside, offsets, 0.0)
    return jnp.where(
        inside, jnp.exp(-math.pi * safe_off * safe_off / (8.0 * spread * spread)), 0.0
    )


def wall_bands(widths_ref, raw_ref, own_ref, edge_ref):
    n_rows = widths_ref.shape[1]
    margin = 2 * WMAX
    block = 64
    count = (n_rows + 2 * margin) // block
    spread = widths_ref[...].astype(jnp.float32)

    def fill(i, total):
        at = pl.multiple_of(i * block, block)
        row = lax.broadcasted_iota(jnp.int32, (block, n_rows), 0) + i * block
        col = lax.broadcasted_iota(jnp.int32, (block, n_rows), 1)
        taps = raw_taps((row - margin - col).astype(jnp.float32), spread)
        raw_ref[pl.ds(at, block), :] = taps
        return total + jnp.sum(taps * taps, axis=0, keepdims=True)

    total = lax.fori_loop(0, count, fill, jnp.zeros((1, n_rows), jnp.float32))
    norm = jnp.sqrt(total)
    edge_ref[:margin, :] = (raw_ref[:margin, :] / norm).astype(jnp.bfloat16)
    own_ref[...] = (raw_ref[margin : margin + n_rows, :] / norm).astype(jnp.bfloat16)
    edge_ref[margin:, :] = (raw_ref[margin + n_rows :, :] / norm).astype(jnp.bfloat16)


def span_band(band_ref):
    n_cols, in_count = band_ref.shape
    margin = 2 * SPANW
    row = lax.broadcasted_iota(jnp.int32, (n_cols, in_count), 0)
    col = lax.broadcasted_iota(jnp.int32, (n_cols, in_count), 1)
    taps = raw_taps((col - margin - row).astype(jnp.float32), float(SPANW))
    norm = jnp.sqrt(jnp.sum(taps * taps, axis=1, keepdims=True))
    band_ref[...] = (taps / norm).astype(jnp.bfloat16)


def filter_kernel(
    n_wall, n_span, noise, widths, fluct, totals,
    stage, spread, psi, halo, smooth, sides, raw, own_band, edge_band, z_band, carry, acc, sums,
    load_sem, spread_sem, meet, wall_send, wall_recv, span_send, span_recv, sum_send, sum_recv,
):
    n_comp, _, n_cols, n_rows = noise.shape
    chunks = stage.shape[0]
    half = n_rows // 2
    moments = acc.shape[0]
    w = lax.axis_index("wall")
    p = lax.axis_index("span")
    left, right = lax.rem(p + n_span - 1, n_span), lax.rem(p + 1, n_span)
    below, above = w > 0, w < n_wall - 1

    barrier = pltpu.get_barrier_semaphore()

    def signal(where, **device):
        pl.semaphore_signal(where, inc=1, device_id=device, device_id_type=MESH)

    signal(barrier, span=left)
    signal(barrier, span=right)

    @pl.when(below)
    def _():
        signal(barrier, wall=w - 1)

    @pl.when(above)
    def _():
        signal(barrier, wall=w + 1)

    n_wall_first = chunks - FIRST
    plain = n_wall_first - FIRST
    early = [k for i in range(FIRST) for k in (n_wall_first + i, i)]

    def time_of(k):
        if isinstance(k, int) and k >= n_wall_first:
            return plain + 1 + 2 * (k - n_wall_first)
        return k + (k // plain) * (k - plain)

    def load(k, sem):
        return pltpu.make_async_copy(
            noise.at[:, pl.ds(time_of(k) * STEP, STEP)], stage.at[k], load_sem.at[sem]
        )

    def start_load(k, _):
        load(k, len(early)).start()
        return 0

    load_spread = pltpu.make_async_copy(widths, spread, spread_sem)
    for sem, k in enumerate(early):
        load(k, sem).start()
    load_spread.start()
    lax.fori_loop(FIRST, n_wall_first, start_load, 0)

    rounds = (n_span // 2).bit_length() - 1

    def reach(r):
        if r < rounds:
            signal(meet.at[r], span=lax.rem(p + 2**r, n_span))
            signal(meet.at[r], span=lax.rem(p + n_span - 2**r, n_span))

    def reached(r):
        if r < rounds:
            pl.semaphore_wait(meet.at[r], 2)

    def to_above(k):
        return pltpu.make_async_remote_copy(
            src_ref=psi.at[k, 1], dst_ref=halo.at[k, 0],
            send_sem=wall_send.at[0], recv_sem=wall_recv.at[k],
            device_id={"wall": w + 1}, device_id_type=MESH,
        )

    def to_below(k):
        return pltpu.make_async_remote_copy(
            src_ref=psi.at[k, 0], dst_ref=halo.at[k, 1],
            send_sem=wall_send.at[1], recv_sem=wall_recv.at[k],
            device_id={"wall": w - 1}, device_id_type=MESH,
        )

    def to_right(k):
        return pltpu.make_async_remote_copy(
            src_ref=smooth.at[k], dst_ref=sides.at[k, 0],
            send_sem=span_send.at[0], recv_sem=span_recv.at[k],
            device_id={"span": right}, device_id_type=MESH,
        )

    def to_left(k):
        return pltpu.make_async_remote_copy(
            src_ref=smooth.at[k], dst_ref=sides.at[k, 1],
            send_sem=span_send.at[1], recv_sem=span_recv.at[k],
            device_id={"span": left}, device_id_type=MESH,
        )

    def landed(ref, sem):
        pltpu.make_async_copy(ref, ref, sem).wait()

    def convert(k, span_first):
        for c in range(n_comp):
            for s in range(STEP):
                bits = stage[k, c, s].astype(jnp.float32)
                field = (math.sqrt(12.0) * ((bits + 0.5) * INV_RANGE - 0.5)).astype(jnp.bfloat16)
                if span_first:
                    smooth[k, c * STEP + s] = field
                else:
                    at = (c * STEP + s) * n_cols
                    psi[k, 0, at : at + n_cols, :] = field[:, :half]
                    psi[k, 1, at : at + n_cols, :] = field[:, half:]

    def send_wall(k):
        @pl.when(above)
        def _():
            to_above(k).start()

        @pl.when(below)
        def _():
            to_below(k).start()

    def send_span(k):
        to_right(k).start()
        to_left(k).start()

    for sem, k in enumerate(early):
        with jax.named_scope("early_convert"):
            load(k, sem).wait()
            convert(k, k >= n_wall_first)
        if sem == 0:
            with jax.named_scope("greeted"):
                pl.semaphore_wait(barrier, 2 + below.astype(jnp.int32) + above.astype(jnp.int32))
        if k >= n_wall_first:
            send_span(k)
        else:
            send_wall(k)

    def convert_and_send(k, _):
        convert(k, False)
        send_wall(k)
        return 0

    reach(0)
    with jax.named_scope("converts"):
        landed(stage.at[pl.ds(FIRST, plain)], load_sem.at[len(early)])
        lax.fori_loop(FIRST, n_wall_first, convert_and_send, 0)
    with jax.named_scope("bands"):
        load_spread.wait()
        wall_bands(spread, raw, own_band, edge_band)
        span_band(z_band)
    carry[...] = jnp.zeros_like(carry)
    acc[...] = jnp.zeros_like(acc)

    @pl.when(jnp.logical_not(below))
    def _():
        def clear(k, _):
            halo[k, 0] = jnp.zeros(halo.shape[2:], halo.dtype)
            return 0

        lax.fori_loop(0, chunks, clear, 0)

    @pl.when(jnp.logical_not(above))
    def _():
        def clear(k, _):
            halo[k, 1] = jnp.zeros(halo.shape[2:], halo.dtype)
            return 0

        lax.fori_loop(0, chunks, clear, 0)

    def wall_arrived(k):
        @pl.when(jnp.logical_and(below, above))
        def _():
            landed(halo.at[k], wall_recv.at[k])

        @pl.when(jnp.logical_not(below))
        def _():
            landed(halo.at[k, 1], wall_recv.at[k])

        @pl.when(jnp.logical_not(above))
        def _():
            landed(halo.at[k, 0], wall_recv.at[k])

    def wall_sum(k):
        with jax.named_scope("wall_wait"):
            wall_arrived(k)
        own = jnp.concatenate([psi[k, 0], psi[k, 1]], axis=1)
        edge = jnp.concatenate([halo[k, 0], halo[k, 1]], axis=1)
        total = jnp.dot(own, own_band[...], preferred_element_type=jnp.float32) + jnp.dot(
            edge, edge_band[...], preferred_element_type=jnp.float32
        )
        return total.reshape(n_comp * STEP, n_cols, n_rows)

    def span_arrived(k):
        with jax.named_scope("span_wait"):
            landed(sides.at[k], span_recv.at[k])

    def span_sum(k, i):
        window = jnp.concatenate([sides[k, 0, i], smooth[k, i], sides[k, 1, i]], axis=0)
        return jnp.dot(z_band[...], window, preferred_element_type=jnp.float32)

    def wall_filter(k):
        smooth[k] = wall_sum(k).astype(jnp.bfloat16)
        send_span(k)

    def span_filter_first(k):
        span_arrived(k)
        for i in range(n_comp * STEP):
            field = span_sum(k, i).astype(jnp.bfloat16)
            psi[k, 0, i * n_cols : (i + 1) * n_cols, :] = field[:, :half]
            psi[k, 1, i * n_cols : (i + 1) * n_cols, :] = field[:, half:]
        send_wall(k)

    def advance(k, filtered):
        for s in range(STEP):
            t = time_of(k) * STEP + s
            fresh = jnp.where(t == 0, 1.0, FRESH)
            values = []
            for c in range(n_comp):
                value = DECAY * carry[c] + fresh * filtered(c, s)
                carry[c] = value
                fluct[c, t] = value
                values.append(value)
            for c in range(n_comp):
                acc[c] += jnp.sum(values[c].reshape(n_cols // 8, 8, n_rows), axis=0)
            for slot, (a, b) in enumerate(PAIRS):
                product = values[a] * values[b]
                acc[n_comp + slot] += jnp.sum(product.reshape(n_cols // 8, 8, n_rows), axis=0)

    def span_filter(k):
        span_arrived(k)
        advance(k, lambda c, s: span_sum(k, c * STEP + s))

    def wall_filter_last(k):
        fields = wall_sum(k)
        for c in range(n_comp):
            for s in range(STEP):
                fluct[c, time_of(k) * STEP + s] = fields[c * STEP + s]

    def middle_steps(k, _):
        wall_filter(k)
        span_filter(k - LAG)
        return 0

    def last_steps(k, _):
        span_filter(k)
        return 0

    for k in range(LAG):
        wall_filter(k)
        if k < FIRST:
            span_filter_first(n_wall_first + k)
        reached(k)
        reach(k + 1)
    lax.fori_loop(LAG, n_wall_first, middle_steps, 0)
    for r in range(LAG, rounds):
        reached(r)
        reach(r + 1)
    lax.fori_loop(n_wall_first - LAG, plain, last_steps, 0)
    for i in range(FIRST):
        wall_filter_last(n_wall_first + i)
        span_filter(plain + i)
        advance(n_wall_first + i, lambda c, s: fluct[c, time_of(n_wall_first + i) * STEP + s])

    for m in range(moments):
        sums[p, m] = jnp.sum(acc[m], axis=0, keepdims=True)

    n_y = min(4, n_span // 2)

    n_x = n_span // (2 * n_y)
    in_group = 2 * n_y
    group = p // in_group

    def rank(there):
        return there // in_group + there // 2 % n_y

    with jax.named_scope("share"):
        for there in sorted(range(n_span), key=rank):

            @pl.when(p != there)
            def _():
                pltpu.make_async_remote_copy(
                    src_ref=sums.at[p], dst_ref=sums.at[p],
                    send_sem=sum_send, recv_sem=sum_recv.at[group],
                    device_id={"span": there}, device_id_type=MESH,
                ).start()

    with jax.named_scope("send_ends"):

        @pl.when(above)
        def _():
            landed(psi.at[:, 1], wall_send.at[0])

        @pl.when(below)
        def _():
            landed(psi.at[:, 0], wall_send.at[1])

        landed(smooth, span_send.at[0])
        landed(smooth, span_send.at[1])

    def collect(i, total):
        return total + sums[i]

    total = jnp.zeros(sums.shape[1:], jnp.float32)
    with jax.named_scope("sums_wait"):
        for g in range(n_x):

            @pl.when(group == g)
            def _():
                landed(sums.at[pl.ds(0, in_group - 1)], sum_recv.at[g])

            @pl.when(group != g)
            def _():
                landed(sums.at[pl.ds(0, in_group)], sum_recv.at[g])

            total = lax.fori_loop(g * in_group, (g + 1) * in_group, collect, total)
    totals[...] = total
    with jax.named_scope("share_ends"):
        landed(sums.at[pl.ds(0, n_span - 1)], sum_send)


def lund_transform(sample_covariance, target_factor_diagonal, target_factor_lower):
    cov_00 = sample_covariance[0] + SPREAD_FLOOR
    cov_10 = sample_covariance[1]
    cov_11 = sample_covariance[2] + SPREAD_FLOOR
    cov_20 = sample_covariance[3]
    cov_21 = sample_covariance[4]
    cov_22 = sample_covariance[5] + SPREAD_FLOOR
    inv_00 = lax.rsqrt(cov_00)
    chol_10 = cov_10 * inv_00
    chol_20 = cov_20 * inv_00
    inv_11 = lax.rsqrt(cov_11 - chol_10 * chol_10)
    chol_21 = (cov_21 - chol_20 * chol_10) * inv_11
    inv_22 = lax.rsqrt(cov_22 - chol_20 * chol_20 - chol_21 * chol_21)
    inv_10 = -chol_10 * inv_00 * inv_11
    inv_21 = -chol_21 * inv_11 * inv_22
    inv_20 = -(chol_20 * inv_00 + chol_21 * inv_10) * inv_22
    gain_00 = target_factor_diagonal[0] * inv_00
    gain_10 = target_factor_lower[0] * inv_00 + target_factor_diagonal[1] * inv_10
    gain_11 = target_factor_diagonal[1] * inv_11
    gain_20 = (
        target_factor_lower[1] * inv_00
        + target_factor_lower[2] * inv_10
        + target_factor_diagonal[2] * inv_20
    )
    gain_21 = target_factor_lower[2] * inv_11 + target_factor_diagonal[2] * inv_21
    gain_22 = target_factor_diagonal[2] * inv_22
    return (gain_00,), (gain_10, gain_11), (gain_20, gain_21, gain_22)


def scale_kernel(cell_count, fluct, totals, profile, diagonal, lower, out, ready, sem):
    n_comp, n_samples, n_cols, n_rows = fluct.shape
    moments = n_comp + len(PAIRS)
    row = [totals[i] * (1.0 / cell_count) for i in range(moments)]
    means = row[:n_comp]
    spread = [row[n_comp + slot] - means[a] * means[b] for slot, (a, b) in enumerate(PAIRS)]
    factors = lund_transform(
        spread,
        [diagonal[i : i + 1, :] for i in range(3)],
        [lower[i : i + 1, :] for i in range(3)],
    )

    def one_sample(s, _):
        centred = [fluct[c, s] - means[c] for c in range(n_comp)]
        for c in range(n_comp):
            value = profile[c : c + 1, :]
            for d in range(c + 1):
                value = value + factors[c][d] * centred[d]
            ready[c, s] = value
        pltpu.make_async_copy(ready.at[:, s], out.at[:, s], sem).start()
        return 0

    lax.fori_loop(0, n_samples, one_sample, 0)
    pltpu.make_async_copy(ready, out, sem).wait()


def shards(
    noise_bits, filter_widths, target_mean_profile, target_factor_diagonal, target_factor_lower
):
    n_comp, n_samples, n_cols, n_rows = noise_bits.shape
    n_wall, n_span = lax.axis_size("wall"), lax.axis_size("span")
    chunks = n_samples // STEP
    rows = n_comp * STEP * n_cols
    half = n_rows // 2
    moments = n_comp + len(PAIRS)
    bf16, f32 = jnp.bfloat16, jnp.float32
    dma = pltpu.SemaphoreType.DMA
    fluct, totals = pl.pallas_call(
        functools.partial(filter_kernel, n_wall, n_span),
        out_shape=(
            pltpu.VMEM((n_comp, n_samples, n_cols, n_rows), f32),
            pltpu.VMEM((moments, 1, n_rows), f32),
        ),
        in_specs=[
            pl.BlockSpec(memory_space=pltpu.HBM),
            pl.BlockSpec(memory_space=pltpu.HBM),
        ],
        out_specs=(
            pl.BlockSpec(memory_space=pltpu.VMEM),
            pl.BlockSpec(memory_space=pltpu.VMEM),
        ),
        scratch_shapes=[
            pltpu.VMEM((chunks, n_comp, STEP, n_cols, n_rows), jnp.int32),
            pltpu.VMEM((1, n_rows), jnp.int32),
            pltpu.VMEM((chunks, 2, rows, half), bf16),
            pltpu.VMEM((chunks, 2, rows, half), bf16),
            pltpu.VMEM((chunks, n_comp * STEP, n_cols, n_rows), bf16),
            pltpu.VMEM((chunks, 2, n_comp * STEP, n_cols, n_rows), bf16),
            pltpu.VMEM((n_rows + 4 * WMAX, n_rows), f32),
            pltpu.VMEM((n_rows, n_rows), bf16),
            pltpu.VMEM((4 * WMAX, n_rows), bf16),
            pltpu.VMEM((n_cols, n_cols + 4 * SPANW), bf16),
            pltpu.VMEM((n_comp, n_cols, n_rows), f32),
            pltpu.VMEM((moments, 8, n_rows), f32),
            pltpu.VMEM((n_span, moments, 1, n_rows), f32),
            dma((2 * FIRST + 1,)),
            dma,
            pltpu.SemaphoreType.REGULAR((max(1, (n_span // 2).bit_length() - 1),)),
            dma((2,)),
            dma((chunks,)),
            dma((2,)),
            dma((chunks,)),
            dma,
            dma((4,)),
        ],
        compiler_params=pltpu.CompilerParams(
            collective_id=0, has_side_effects=True, vmem_limit_bytes=40 * 1024 * 1024
        ),
        name="filters",
    )(
        pltpu.with_memory_space_constraint(noise_bits, pltpu.HBM),
        pltpu.with_memory_space_constraint(filter_widths.reshape(1, n_rows), pltpu.HBM),
    )

    in_vmem = pl.BlockSpec(memory_space=pltpu.VMEM)
    return pl.pallas_call(
        functools.partial(scale_kernel, float(n_samples * n_cols * n_span)),
        out_shape=pltpu.HBM(noise_bits.shape, f32),
        in_specs=[in_vmem] * 5,
        out_specs=pl.BlockSpec(memory_space=pltpu.HBM),
        scratch_shapes=[pltpu.VMEM(noise_bits.shape, f32), dma],
        compiler_params=pltpu.CompilerParams(vmem_limit_bytes=16 * 1024 * 1024),
        name="rescale",
    )(fluct, totals, target_mean_profile, target_factor_diagonal, target_factor_lower)


def solution(mesh):
    placed = (
        P(None, None, "span", "wall"),
        P("wall"),
        P(None, "wall"),
        P(None, "wall"),
        P(None, "wall"),
    )
    return jax.shard_map(
        shards, mesh=mesh, in_specs=placed, out_specs=P(None, None, "span", "wall"), check_vma=False
    )
```
